256 devices in a mesh: section: 8 (over y, core), replica: 32 (over z, x).
Axes of the slice: x: 4, y: 4, z: 8, core: 2. Of those that a mesh axis runs over, the one named last changes fastest.
Arguments:
- gradient: bfloat16 [1024, 131072], P('section', 'replica'), may hold values from -1300 to 1300
- residual: float32 [1024, 131072], P('section', 'replica'), may hold values from -6 to 6
- block_ids: int32 [8, 256], P('section', 'replica'), may hold values from 0 to 15, as said below
- block_counts: int32 [8, 32], P('section', 'replica'), may hold values from 1 to 8, as said below
Outputs:
- new_residual: float32 [1024, 131072], P('section', 'replica')
- update: bfloat16 [1024, 4096], P('section', 'replica')
The draws below stay inside these ranges and needn't reach their ends.
Inputs may be any that keep to these rules, and one draw needn't show every extreme that they name: `block_ids`: each device's 8 block numbers are distinct; only the first block_counts of them are selected. `block_counts`: in every section some replica selects exactly 8 blocks; the others select at most 4.
All inputs are finite; a program needn't handle non-finite values.
Results may differ from the reference program's by a relative error of at most 0.013.
Values may be sent and summed in bfloat16 or wider, within the bound.
A program may use at most 64 MiB of HBM per device.

```python
import math
import jax
import jax.numpy as jnp
from jax import lax

D = 4096
ROWS = 128
BLK = 8
KMAX = 8
SECTIONS = 8
REPLICAS = 32


def draw_gradient(key, part):
    key_rows, key_base, key_common, key_level, key_mix, key_slice, key_column = jax.random.split(key, 7)
    slice_width = D // REPLICAS
    row_scale = jnp.exp(jax.random.uniform(key_rows, (SECTIONS * ROWS, REPLICAS, 1), jnp.float32, 0.0, math.log(10.0)))
    section_of_row = (jnp.arange(SECTIONS * ROWS, dtype=jnp.int32) // ROWS).astype(jnp.int32)
    section_scale = 1.0 + 2.0 * section_of_row.astype(jnp.float32) / max(SECTIONS - 1, 1)
    slice_of_column = (jnp.arange(D, dtype=jnp.int32) // slice_width).astype(jnp.int32)
    slice_scale = jnp.exp(jax.random.uniform(key_slice, (REPLICAS,), jnp.float32, 0.0, math.log(4.0)))
    column_rough = jax.random.uniform(key_column, (D,), jnp.float32, 0.6, 1.4)
    column_scale = slice_scale[slice_of_column] * column_rough
    section_level = jax.random.uniform(key_level, (SECTIONS,), jnp.float32, 0.0, 1.2)
    slice_mix = jax.random.uniform(key_mix, (SECTIONS, REPLICAS), jnp.float32, 0.0, 1.0)
    mix_weight = section_level[:, None] * slice_mix
    weight_grid = mix_weight[section_of_row][:, slice_of_column]
    base_draw = jnp.clip(jax.random.normal(key_base, (SECTIONS * ROWS, REPLICAS, D), jnp.float32), -4.0, 4.0)
    common_part = jnp.clip(jax.random.normal(key_common, (SECTIONS * ROWS, 1, D), jnp.float32), -3.0, 3.0)
    base_draw = base_draw + weight_grid[:, None, :] * common_part
    values = base_draw * row_scale * section_scale[:, None, None] * column_scale[None, None, :]
    return values.reshape(SECTIONS * ROWS, REPLICAS * D).astype(jnp.bfloat16)


def draw_block_ids(key, part):
    block_total = ROWS // BLK
    scores = jax.random.randint(key, (SECTIONS, REPLICAS, block_total), 0, 1 << 20) * block_total + jnp.arange(block_total, dtype=jnp.int32)
    ordering = jnp.argsort(scores, axis=-1, stable=True)
    return ordering[..., :KMAX].reshape(SECTIONS, REPLICAS * KMAX).astype(jnp.int32)


def draw_block_counts(key, part):
    key_base, key_busy = jax.random.split(key)
    base_draw = jax.random.randint(key_base, (SECTIONS, REPLICAS), 1, KMAX // 2 + 1)
    busy_replica = jax.random.randint(key_busy, (SECTIONS, 1), 0, REPLICAS)
    placed = jnp.arange(REPLICAS, dtype=jnp.int32)[None, :] == busy_replica
    return jnp.where(placed, KMAX, base_draw).astype(jnp.int32)


def block_scale(stream_key, extent, cuts, low, top_value):
    level, own = 1.0, jax.random.fold_in(stream_key, 6)
    for axis_at, shards_of in cuts:
        draws = jnp.exp(jax.random.uniform(jax.random.fold_in(own, axis_at), (shards_of,), jnp.float32, low / len(cuts), top_value / len(cuts)))
        level = level * jnp.repeat(draws, extent[axis_at] // shards_of).reshape([-1 if axis == axis_at else 1 for axis in range(len(extent))])
    return level


def centred(rng, dims, scale, reach, shards=(), kind=jnp.bfloat16):
    array = scale * jax.random.normal(rng, dims, jnp.float32)
    if shards:
        array = array * block_scale(rng, dims, shards, -0.22, 0.18)
    return jnp.clip(array, -reach, reach).astype(kind)


def setup_inputs(seed: int = 0) -> dict:
    streams_of = jax.random.split(jax.random.key(seed), 5)
    gradient = draw_gradient(jax.random.fold_in(streams_of[4], 71), 0)
    residual = centred(streams_of[1], (SECTIONS * ROWS, REPLICAS * D), 1.0, 6.0, ((0, 8), (1, 32)), jnp.float32)
    block_ids = draw_block_ids(jax.random.fold_in(streams_of[4], 71), 0)
    block_counts = draw_block_counts(jax.random.fold_in(streams_of[4], 71), 0)
    return dict(gradient=gradient, residual=residual, block_ids=block_ids, block_counts=block_counts)


scale_level = 1.0
epsilon = 1e-06

def reference(gradient, residual, block_ids, block_counts):
    block_total = ROWS // BLK
    accumulated = gradient.astype(jnp.float32) + residual
    slot_ids = block_ids.reshape(SECTIONS, REPLICAS, KMAX)
    live_slot = jnp.arange(KMAX, dtype=jnp.int32)[None, None, :] < block_counts[:, :, None]
    hit_table = (slot_ids[..., None] == jnp.arange(block_total, dtype=jnp.int32)) & live_slot[..., None]
    chosen = jnp.any(hit_table, axis=2)
    block_mask = jnp.transpose(chosen, (0, 2, 1))[:, :, None, :, None]
    shaped = accumulated.reshape(SECTIONS, block_total, BLK, REPLICAS, D)
    sent = jnp.where(block_mask, shaped.astype(jnp.bfloat16).astype(jnp.float32), jnp.float32(0.0))
    new_residual = (shaped - sent).reshape(accumulated.shape)
    summed = lax.optimization_barrier(jnp.sum(sent, axis=3)).reshape(SECTIONS * ROWS, D)
    norm_total = jnp.sum(summed * summed)
    root_mean = jnp.sqrt(norm_total / (SECTIONS * ROWS * D) + epsilon)
    clip_factor = scale_level / root_mean
    update = (summed * clip_factor).astype(jnp.bfloat16)
    return (new_residual, update)
```

```python
import functools
import jax
import jax.numpy as jnp
from jax import lax
from jax.experimental import pallas as pl
from jax.experimental.pallas import tpu as pltpu
from jax.sharding import PartitionSpec as P

BLK = 8
LANES = 128
MESH = pl.DeviceIdType.MESH

scale_level = 1.0
epsilon = 1e-06


def plane_order(nz, nx):
    offsets = [(dz, dx) for dz in range(nz) for dx in range(nx) if (dz, dx) != (0, 0)]
    far = lambda d, n: min(d, n - d)
    return sorted(offsets, key=lambda o: (-far(o[0], nz) - far(o[1], nx), far(o[1], nx), o))


def kernel(
    nz, nx, sections, count_total,
    grad_hbm, res_hbm, ids_ref, count_ref,
    new_res, update,
    grad, res, packed, rows_out, recv, rows_in, sums, sums_a, sums_b,
    load_sem, data_send, data_recv, rows_send, rows_recv, a_send, a_recv, b_send, b_recv,
):
    replicas = nz * nx
    blocks, _, width = grad.shape
    row_count = blocks * BLK
    cols = width // replicas
    slots = ids_ref.shape[1]
    sec, rep = lax.axis_index("section"), lax.axis_index("replica")
    z, x = rep // nx, rep % nx

    loads = []
    chunks = 4
    step = blocks // chunks
    for c in range(chunks):
        part = pl.ds(c * step, step)
        pair = (
            pltpu.make_async_copy(grad_hbm.at[part], grad.at[part], load_sem.at[0, c]),
            pltpu.make_async_copy(res_hbm.at[part], res.at[part], load_sem.at[1, c]),
        )
        for copy in pair:
            copy.start()
        loads.append(pair)

    plane = []
    for dz, dx in plane_order(nz, nx):
        plane.append(((z + dz) % nz) * nx + (x + dx) % nx)
    across = [(sec + d) % sections for d in range(1, sections)]
    barrier = pltpu.get_barrier_semaphore()
    for peer in plane:
        pl.semaphore_signal(barrier, inc=1, device_id=(sec, peer), device_id_type=MESH)
    for peer in across:
        pl.semaphore_signal(barrier, inc=1, device_id=(peer, rep), device_id_type=MESH)

    lane = lax.broadcasted_iota(jnp.int32, (1, LANES), 1)
    half = rep % 2
    slot_of = lane // BLK - half * slots
    count = jnp.full((1, LANES), count_ref[0, 0], jnp.int32)
    ids = [jnp.full((1, LANES), ids_ref[0, s], jnp.int32) for s in range(slots)]
    ids = [jnp.where(count > s, ids[s], -1) for s in range(slots)]
    target = jnp.full((1, LANES), -1, jnp.int32)
    for s in range(slots):
        target = jnp.where(slot_of == s, ids[s] * BLK + lane % BLK, target)
    rows_out[0] = target
    rows_in[pl.ds(rep, 1)] = target[None]

    per_chunk = blocks // chunks
    for c in range(chunks):
        for copy in loads[c]:
            copy.wait()
        for b in range(c * per_chunk, (c + 1) * per_chunk):
            mine = grad[b].astype(jnp.float32) + res[b]
            res[b] = mine
            hit = jnp.zeros((1, LANES), jnp.float32)
            for s in range(slots):
                hit = jnp.where(ids[s] == b, 1.0, hit)
            kept = jnp.concatenate([jnp.broadcast_to(hit, (BLK, LANES))] * (width // LANES), axis=1)
            new_res[b] = mine - mine.astype(jnp.bfloat16).astype(jnp.float32) * kept

    for pair in range(slots // 2):
        picked = [res[ids_ref[0, 2 * pair + h]] for h in range(2)]
        both = jnp.concatenate(picked, axis=0).astype(jnp.bfloat16)
        for r in range(replicas):
            packed[r, pair * 2 * BLK : (pair + 1) * 2 * BLK, :] = both[:, r * cols : (r + 1) * cols]

    pl.semaphore_wait(barrier, len(plane) + len(across))

    for peer in plane:
        pltpu.make_async_remote_copy(
            rows_out.at[0], rows_in.at[rep], rows_send, rows_recv, device_id=(sec, peer), device_id_type=MESH
        ).start()
    for peer in plane:
        pltpu.make_async_remote_copy(
            packed.at[peer], recv.at[rep], data_send, data_recv, device_id=(sec, peer), device_id_type=MESH
        ).start()
    recv[pl.ds(rep, 1)] = packed[pl.ds(rep, 1)]

    others = replicas - 1
    every = rows_in.at[pl.ds(0, others)]
    pltpu.make_async_copy(every, every, rows_recv).wait()
    every = recv.at[pl.ds(0, others)]
    pltpu.make_async_copy(every, every, data_recv).wait()

    row = lax.broadcasted_iota(jnp.int32, (row_count, LANES), 0)
    summed = jnp.zeros((row_count, cols), jnp.float32)
    for pair in range(replicas // 2):
        first, second = rows_in[2 * pair], rows_in[2 * pair + 1]
        lanes = lax.broadcasted_iota(jnp.int32, (1, LANES), 1)
        both = jnp.where(lanes < slots * BLK, first, second)
        hot = jnp.where(row == both, 1.0, 0.0).astype(jnp.bfloat16)
        held = recv[2 * pair : 2 * pair + 2].reshape(2 * slots * BLK, cols)
        summed = summed + jnp.dot(hot, held, preferred_element_type=jnp.float32)

    square = (summed * summed).reshape(row_count // 8, 8, cols).sum(axis=0).sum(axis=0, keepdims=True)
    sums[0] = square
    sums_a[pl.ds(rep, 1)] = square[None]
    for peer in plane:
        pltpu.make_async_remote_copy(
            sums.at[0], sums_a.at[rep], a_send, a_recv, device_id=(sec, peer), device_id_type=MESH
        ).start()
    every = sums_a.at[pl.ds(0, others)]
    pltpu.make_async_copy(every, every, a_recv).wait()
    of_plane = sums_a[...].reshape(replicas, cols).sum(axis=0, keepdims=True)
    sums[1] = of_plane
    sums_b[pl.ds(sec, 1)] = of_plane[None]
    for peer in across:
        pltpu.make_async_remote_copy(
            sums.at[1], sums_b.at[sec], b_send, b_recv, device_id=(peer, rep), device_id_type=MESH
        ).start()
    every = sums_b.at[pl.ds(0, sections - 1)]
    pltpu.make_async_copy(every, every, b_recv).wait()
    of_all = sums_b[...].reshape(sections, cols).sum(axis=0, keepdims=True).sum(axis=1, keepdims=True)
    clip_factor = scale_level / jnp.sqrt(of_all / count_total + epsilon)
    update[...] = (summed * clip_factor).astype(jnp.bfloat16)

    every = packed.at[pl.ds(0, others)]
    pltpu.make_async_copy(every, every, data_send).wait()
    every = rows_in.at[pl.ds(0, others)]
    pltpu.make_async_copy(every, every, rows_send).wait()
    every = sums_a.at[pl.ds(0, others)]
    pltpu.make_async_copy(every, every, a_send).wait()
    every = sums_b.at[pl.ds(0, sections - 1)]
    pltpu.make_async_copy(every, every, b_send).wait()


def per_device(nz, nx, sections, gradient, residual, block_ids, block_counts):
    replicas = nz * nx
    row_count, width = gradient.shape
    cols = width // replicas
    slots = block_ids.shape[1]
    count_total = sections * row_count * width
    f32, bf16, i32 = jnp.float32, jnp.bfloat16, jnp.int32
    dma = pltpu.SemaphoreType.DMA
    blocks = row_count // BLK
    shape = (blocks, BLK, width)
    new_residual, update = pl.pallas_call(
        functools.partial(kernel, nz, nx, sections, count_total),
        out_shape=(
            OUT(shape, f32),
            OUT((row_count, cols), bf16),
        ),
        in_specs=[
            pl.BlockSpec(memory_space=pl.ANY),
            pl.BlockSpec(memory_space=pl.ANY),
            pl.BlockSpec(memory_space=pltpu.SMEM),
            pl.BlockSpec(memory_space=pltpu.SMEM),
        ],
        out_specs=(
            pl.BlockSpec(memory_space=pltpu.VMEM),
            pl.BlockSpec(memory_space=pltpu.VMEM),
        ),
        scratch_shapes=[
            pltpu.VMEM(shape, bf16),
            pltpu.VMEM(shape, f32),
            pltpu.VMEM((replicas, slots * BLK, cols), bf16),
            pltpu.VMEM((1, 1, LANES), i32),
            pltpu.VMEM((replicas, slots * BLK, cols), bf16),
            pltpu.VMEM((replicas, 1, LANES), i32),
            pltpu.VMEM((2, 1, cols), f32),
            pltpu.VMEM((replicas, 1, cols), f32),
            pltpu.VMEM((sections, 1, cols), f32),
            dma((2, 4)), dma, dma, dma, dma, dma, dma, dma, dma,
        ],
        compiler_params=pltpu.CompilerParams(
            collective_id=0, has_side_effects=True
        ),
    )(gradient.reshape(shape), residual.reshape(shape), block_ids, block_counts)
    return new_residual.reshape(row_count, width), update


OUT = jax.ShapeDtypeStruct


def solution(mesh):
    sections, replicas = mesh.shape["section"], mesh.shape["replica"]
    nx = 4
    nz = replicas // nx
    both = P("section", "replica")
    return jax.shard_map(
        functools.partial(per_device, nz, nx, sections),
        mesh=mesh,
        in_specs=(both, both, both, both),
        out_specs=(both, both),
        check_vma=False,
    )
```

```python
import functools
import jax
import jax.numpy as jnp
from jax import lax
from jax.experimental import pallas as pl
from jax.experimental.pallas import tpu as pltpu
from jax.sharding import PartitionSpec as P

BLK = 8
LANES = 128
NX = 4
DIRECT = 4
MESH = pl.DeviceIdType.MESH

scale_level = 1.0
epsilon = 1e-06


def ring_far(d, n):
    return min(d, n - d)


def plane_order(nz, nx):
    offsets = [(dz, dx) for dz in range(nz) for dx in range(nx) if (dz, dx) != (0, 0)]
    return sorted(
        offsets, key=lambda o: (-ring_far(o[0], nz) - ring_far(o[1], nx), ring_far(o[1], nx), o)
    )


def kernel(
    nz, nx, sections, count_total,
    grad_hbm, res_hbm, ids_ref, count_ref,
    new_res, update,
    grad, res, packed, packed_ext, rows_out, recv, recv_ext, merged, recv_merged, rows_in, square_out, squares,
    load_sem, data_send, data_recv, rows_send, rows_recv, ext_send, ext_recv, merged_send, merged_recv,
    square_send, square_recv,
):
    replicas = nz * nx
    blocks, _, width = grad.shape
    row_count = blocks * BLK
    cols = width // replicas
    slots = ids_ref.shape[1]
    sec, rep = lax.axis_index("section"), lax.axis_index("replica")
    z, x = rep // nx, rep % nx
    others = replicas - 1
    f32, bf16 = jnp.float32, jnp.bfloat16

    loads = []
    chunks = 4
    step = blocks // chunks
    for c in range(chunks):
        part = pl.ds(c * step, step)
        pair = (
            pltpu.make_async_copy(grad_hbm.at[part], grad.at[part], load_sem.at[0, c]),
            pltpu.make_async_copy(res_hbm.at[part], res.at[part], load_sem.at[1, c]),
        )
        for copy in pair:
            copy.start()
        loads.append(pair)

    order = plane_order(nz, nx)
    peer_of = {(dz, dx): ((z + dz) % nz) * nx + (x + dx) % nx for dz, dx in order}
    across = [(sec + d) % sections for d in range(1, sections)]
    barrier = pltpu.get_barrier_semaphore()
    for o in order:
        pl.semaphore_signal(barrier, inc=1, device_id=(sec, peer_of[o]), device_id_type=MESH)
    for peer in across:
        pl.semaphore_signal(barrier, inc=1, device_id=(peer, rep), device_id_type=MESH)

    lane = lax.broadcasted_iota(jnp.int32, (1, LANES), 1)
    group = LANES // (DIRECT * BLK)
    slot_of = lane // BLK - (rep % group) * DIRECT
    count = jnp.full((1, LANES), count_ref[0, 0], jnp.int32)
    ids = [jnp.full((1, LANES), ids_ref[0, s], jnp.int32) for s in range(slots)]
    ids = [jnp.where(count > s, ids[s], -1) for s in range(slots)]
    direct_row = jnp.zeros((1, LANES), jnp.int32)
    ext_row = jnp.zeros((1, LANES), jnp.int32)
    for s in range(slots):
        target = jnp.where(ids[s] >= 0, ids[s] * BLK + lane % BLK + 1, 0)
        if s < DIRECT:
            direct_row = jnp.where(slot_of == s, target, direct_row)
        else:
            ext_row = jnp.where(lane // BLK == s - DIRECT, target, ext_row)
    both_rows = jnp.concatenate([direct_row, ext_row], axis=0)
    rows_out[0] = both_rows
    rows_in[pl.ds(rep, 1)] = both_rows[None]

    for c in range(chunks):
        for copy in loads[c]:
            copy.wait()
        for b in range(c * step, (c + 1) * step):
            res[b] = grad[b].astype(f32) + res[b]

    shift = nz // 2 + 1
    far_steps = 3
    for pair in range(DIRECT // 2, slots // 2):
        picked = []
        for h in range(2):
            s = 2 * pair + h
            alive = jnp.broadcast_to(jnp.where(ids[s] >= 0, 1.0, 0.0), (BLK, LANES))
            alive = jnp.concatenate([alive] * (width // LANES), axis=1)
            picked.append(jnp.where(alive > 0.5, res[ids_ref[0, s]], 0.0))
        both = jnp.concatenate(picked, axis=0).astype(bf16)
        rows = slice((pair - DIRECT // 2) * 2 * BLK, (pair - DIRECT // 2 + 1) * 2 * BLK)
        for zd in range(nz):
            place = (zd - z + shift + nz) % nz
            for xd in range(nx):
                r = zd * nx + xd
                packed_ext[xd, pl.ds(place, 1), rows, :] = both[None, :, r * cols : (r + 1) * cols]
    for pair in range(DIRECT // 2):
        both = jnp.concatenate([res[ids_ref[0, 2 * pair + h]] for h in range(2)], axis=0).astype(bf16)
        rows = slice(pair * 2 * BLK, (pair + 1) * 2 * BLK)
        for r in range(replicas):
            packed[r, rows, :] = both[:, r * cols : (r + 1) * cols]
    recv[pl.ds(rep, 1)] = packed[pl.ds(rep, 1)]
    recv_ext[pl.ds(x, 1)] = packed_ext[pl.ds(x, 1)]

    pl.semaphore_wait(barrier, len(order) + len(across))

    halves = (pl.ds(0, far_steps), pl.ds(far_steps, nz - far_steps))
    for h in range(2):
        for dx in sorted(range(1, nx), key=lambda d: -ring_far(d, nx)):
            xd = (x + dx) % nx
            pltpu.make_async_remote_copy(
                packed_ext.at[xd, halves[h]], recv_ext.at[x, halves[h]], ext_send.at[h], ext_recv.at[h],
                device_id=(sec, z * nx + xd), device_id_type=MESH,
            ).start()
    for o in order:
        pltpu.make_async_remote_copy(
            rows_out.at[0], rows_in.at[rep], rows_send, rows_recv, device_id=(sec, peer_of[o]), device_id_type=MESH
        ).start()

    def send_direct(lengths):
        for o in order:
            if ring_far(o[0], nz) in lengths:
                pltpu.make_async_remote_copy(
                    packed.at[peer_of[o]], recv.at[rep], data_send, data_recv,
                    device_id=(sec, peer_of[o]), device_id_type=MESH,
                ).start()

    def forward(h):
        places = range(far_steps) if h == 0 else range(far_steps, nz)
        every = recv_ext.at[pl.ds(0, nx - 1), halves[h]]
        pltpu.make_async_copy(every, every, ext_recv.at[h]).wait()
        total = recv_ext[0, places[0] : places[-1] + 1]
        for k in range(1, nx):
            total = total + recv_ext[k, places[0] : places[-1] + 1]
        merged[places[0] : places[-1] + 1] = total
        for place in sorted(places, key=lambda p: -ring_far((p - shift) % nz, nz)):
            dz = (place - shift) % nz
            if dz:
                pltpu.make_async_remote_copy(
                    merged.at[place], recv_merged.at[z], merged_send, merged_recv,
                    device_id=(sec, ((z + dz) % nz) * nx + x), device_id_type=MESH,
                ).start()
            else:
                recv_merged[pl.ds(z, 1)] = total[place - places[0] : place - places[0] + 1]

    send_direct((3, 4))
    forward(0)
    send_direct((2,))
    forward(1)
    send_direct((1, 0))

    for b in range(blocks):
        hit = jnp.zeros((1, LANES), f32)
        for s in range(slots):
            hit = jnp.where(ids[s] == b, 1.0, hit)
        kept = jnp.concatenate([jnp.broadcast_to(hit, (BLK, LANES))] * (width // LANES), axis=1)
        mine = res[b]
        new_res[b] = mine - mine.astype(bf16).astype(f32) * kept

    every = rows_in.at[pl.ds(0, others)]
    pltpu.make_async_copy(every, every, rows_recv).wait()
    row = lax.broadcasted_iota(jnp.int32, (row_count, LANES), 0) + 1
    ext_rows = rows_in[0][1:2]
    for r in range(1, replicas):
        ext_rows = ext_rows + rows_in[r][1:2]
    hot_ext = jnp.where(row == ext_rows, 1.0, 0.0).astype(bf16)[:, : (slots - DIRECT) * BLK]
    hots = []
    for g in range(replicas // group):
        rows = rows_in[g * group][0:1]
        for k in range(1, group):
            rows = rows + rows_in[g * group + k][0:1]
        hots.append(jnp.where(row == rows, 1.0, 0.0).astype(bf16))

    every = recv.at[pl.ds(0, others)]
    pltpu.make_async_copy(every, every, data_recv).wait()
    every = recv_merged.at[pl.ds(0, nz - 1)]
    pltpu.make_async_copy(every, every, merged_recv).wait()

    ext = recv_merged[0]
    for k in range(1, nz):
        ext = ext + recv_merged[k]
    summed = jnp.dot(hot_ext, ext, preferred_element_type=f32)
    for g, hot in enumerate(hots):
        held = recv[g * group : (g + 1) * group].reshape(LANES, cols)
        summed = summed + jnp.dot(hot, held, preferred_element_type=f32)

    square = (summed * summed).reshape(row_count // 8, 8, cols).sum(axis=0).sum(axis=0, keepdims=True)
    device = sec * replicas + rep
    square_out[0] = square
    squares[pl.ds(device, 1)] = square[None]
    for o in order:
        for d in range(sections):
            pltpu.make_async_remote_copy(
                square_out.at[0], squares.at[device], square_send, square_recv,
                device_id=((sec + d) % sections, peer_of[o]), device_id_type=MESH,
            ).start()
    for peer in across:
        pltpu.make_async_remote_copy(
            square_out.at[0], squares.at[device], square_send, square_recv,
            device_id=(peer, rep), device_id_type=MESH,
        ).start()
    every_square = squares.at[pl.ds(0, sections * replicas - 1)]
    pltpu.make_async_copy(every_square, every_square, square_recv).wait()
    of_all = squares[...].sum(axis=0).sum(axis=1, keepdims=True)
    clip_factor = scale_level / jnp.sqrt(of_all / count_total + epsilon)
    update[...] = (summed * clip_factor).astype(bf16)

    every = packed.at[pl.ds(0, others)]
    pltpu.make_async_copy(every, every, data_send).wait()
    every = rows_in.at[pl.ds(0, others)]
    pltpu.make_async_copy(every, every, rows_send).wait()
    for h in range(2):
        every = recv_ext.at[pl.ds(0, nx - 1), halves[h]]
        pltpu.make_async_copy(every, every, ext_send.at[h]).wait()
    every = recv_merged.at[pl.ds(0, nz - 1)]
    pltpu.make_async_copy(every, every, merged_send).wait()
    pltpu.make_async_copy(every_square, every_square, square_send).wait()


def per_device(nz, nx, sections, gradient, residual, block_ids, block_counts):
    replicas = nz * nx
    row_count, width = gradient.shape
    cols = width // replicas
    slots = block_ids.shape[1]
    count_total = sections * row_count * width
    f32, bf16, i32 = jnp.float32, jnp.bfloat16, jnp.int32
    dma = pltpu.SemaphoreType.DMA
    blocks = row_count // BLK
    shape = (blocks, BLK, width)
    direct_rows, ext_rows = DIRECT * BLK, (slots - DIRECT) * BLK
    new_residual, update = pl.pallas_call(
        functools.partial(kernel, nz, nx, sections, count_total),
        out_shape=(pltpu.VMEM(shape, f32), pltpu.VMEM((row_count, cols), bf16)),
        in_specs=[
            pl.BlockSpec(memory_space=pl.ANY),
            pl.BlockSpec(memory_space=pl.ANY),
            pl.BlockSpec(memory_space=pltpu.SMEM),
            pl.BlockSpec(memory_space=pltpu.SMEM),
        ],
        out_specs=(
            pl.BlockSpec(memory_space=pltpu.VMEM),
            pl.BlockSpec(memory_space=pltpu.VMEM),
        ),
        scratch_shapes=[
            pltpu.VMEM(shape, bf16),
            pltpu.VMEM(shape, f32),
            pltpu.VMEM((replicas, direct_rows, cols), bf16),
            pltpu.VMEM((nx, nz, ext_rows, cols), bf16),
            pltpu.VMEM((1, 2, LANES), i32),
            pltpu.VMEM((replicas, direct_rows, cols), bf16),
            pltpu.VMEM((nx, nz, ext_rows, cols), bf16),
            pltpu.VMEM((nz, ext_rows, cols), bf16),
            pltpu.VMEM((nz, ext_rows, cols), bf16),
            pltpu.VMEM((replicas, 2, LANES), i32),
            pltpu.VMEM((1, 1, cols), f32),
            pltpu.VMEM((sections * replicas, 1, cols), f32),
            dma((2, 4)), dma, dma, dma, dma, dma((2,)), dma((2,)), dma, dma, dma, dma,
        ],
        compiler_params=pltpu.CompilerParams(collective_id=0, has_side_effects=True),
    )(gradient.reshape(shape), residual.reshape(shape), block_ids, block_counts)
    return new_residual.reshape(row_count, width), update


def solution(mesh):
    sections, replicas = mesh.shape["section"], mesh.shape["replica"]
    both = P("section", "replica")
    return jax.shard_map(
        functools.partial(per_device, replicas // NX, NX, sections),
        mesh=mesh,
        in_specs=(both, both, both, both),
        out_specs=(both, both),
        check_vma=False,
    )
```

```python
import functools
import jax
import jax.numpy as jnp
from jax import lax
from jax.experimental import pallas as pl
from jax.experimental.pallas import tpu as pltpu
from jax.sharding import PartitionSpec as P

BLK = 8
LANES = 128
NX = 4
DIRECT = 4
MESH = pl.DeviceIdType.MESH

scale_level = 1.0
epsilon = 1e-06


def ring_far(d, n):
    return min(d, n - d)


def plane_order(nz, nx):
    offsets = [(dz, dx) for dz in range(nz) for dx in range(nx) if (dz, dx) != (0, 0)]
    return sorted(
        offsets, key=lambda o: (-ring_far(o[0], nz) - ring_far(o[1], nx), ring_far(o[1], nx), o)
    )


def kernel(
    nz, nx, sections,
    grad_hbm, res_hbm, ids_ref, count_ref,
    new_res, summed_out, squares,
    grad, res, packed, packed_ext, rows_out, recv, recv_ext, merged, recv_merged, rows_in, square_out,
    load_sem, data_send, data_recv, rows_send, rows_recv, ext_send, ext_recv, merged_send, merged_recv,
    square_send, square_recv,
):
    replicas = nz * nx
    blocks, _, width = grad.shape
    row_count = blocks * BLK
    cols = width // replicas
    slots = ids_ref.shape[1]
    sec, rep = lax.axis_index("section"), lax.axis_index("replica")
    z, x = rep // nx, rep % nx
    others = replicas - 1
    f32, bf16 = jnp.float32, jnp.bfloat16

    loads = []
    chunks = 4
    step = blocks // chunks
    for c in range(chunks):
        part = pl.ds(c * step, step)
        pair = (
            pltpu.make_async_copy(grad_hbm.at[part], grad.at[part], load_sem.at[0, c]),
            pltpu.make_async_copy(res_hbm.at[part], res.at[part], load_sem.at[1, c]),
        )
        for copy in pair:
            copy.start()
        loads.append(pair)

    order = plane_order(nz, nx)
    peer_of = {(dz, dx): ((z + dz) % nz) * nx + (x + dx) % nx for dz, dx in order}
    across = [(sec + d) % sections for d in range(1, sections)]
    barrier = pltpu.get_barrier_semaphore()
    for o in order:
        pl.semaphore_signal(barrier, inc=1, device_id=(sec, peer_of[o]), device_id_type=MESH)
    for peer in across:
        pl.semaphore_signal(barrier, inc=1, device_id=(peer, rep), device_id_type=MESH)

    lane = lax.broadcasted_iota(jnp.int32, (1, LANES), 1)
    group = LANES // (DIRECT * BLK)
    slot_of = lane // BLK - (rep % group) * DIRECT
    count = jnp.full((1, LANES), count_ref[0, 0], jnp.int32)
    ids = [jnp.full((1, LANES), ids_ref[0, s], jnp.int32) for s in range(slots)]
    ids = [jnp.where(count > s, ids[s], -1) for s in range(slots)]
    base = 2 * row_count
    both_rows = jnp.zeros((1, LANES), jnp.int32)
    for s in range(slots):
        target = jnp.where(ids[s] >= 0, ids[s] * BLK + lane % BLK + 1, 0)
        if s < DIRECT:
            both_rows = both_rows + jnp.where(slot_of == s, target, 0)
        else:
            both_rows = both_rows + jnp.where(slot_of == s - DIRECT, target * base, 0)
    rows_out[...] = both_rows
    rows_in[pl.ds(rep, 1)] = both_rows

    for c in range(chunks):
        for copy in loads[c]:
            copy.wait()
        for b in range(c * step, (c + 1) * step):
            res[b] = grad[b].astype(f32) + res[b]

    shift = nz // 2 + 1
    far_steps = 3
    for pair in range(DIRECT // 2, slots // 2):
        picked = []
        for h in range(2):
            s = 2 * pair + h
            alive = jnp.broadcast_to(jnp.where(ids[s] >= 0, 1.0, 0.0), (BLK, LANES))
            alive = jnp.concatenate([alive] * (width // LANES), axis=1)
            picked.append(jnp.where(alive > 0.5, res[ids_ref[0, s]], 0.0))
        both = jnp.concatenate(picked, axis=0).astype(bf16)
        rows = slice((pair - DIRECT // 2) * 2 * BLK, (pair - DIRECT // 2 + 1) * 2 * BLK)
        for zd in range(nz):
            place = (zd - z + shift + nz) % nz
            for xd in range(nx):
                r = zd * nx + xd
                packed_ext[xd, pl.ds(place, 1), rows, :] = both[None, :, r * cols : (r + 1) * cols]
    for pair in range(DIRECT // 2):
        both = jnp.concatenate([res[ids_ref[0, 2 * pair + h]] for h in range(2)], axis=0).astype(bf16)
        rows = slice(pair * 2 * BLK, (pair + 1) * 2 * BLK)
        for r in range(replicas):
            packed[r, rows, :] = both[:, r * cols : (r + 1) * cols]
    recv[pl.ds(rep, 1)] = packed[pl.ds(rep, 1)]
    recv_ext[pl.ds(x, 1)] = packed_ext[pl.ds(x, 1)]

    pl.semaphore_wait(barrier, len(order) + len(across))

    halves = (pl.ds(0, far_steps), pl.ds(far_steps, nz - far_steps))
    for h in range(2):
        for dx in sorted(range(1, nx), key=lambda d: -ring_far(d, nx)):
            xd = (x + dx) % nx
            pltpu.make_async_remote_copy(
                packed_ext.at[xd, halves[h]], recv_ext.at[x, halves[h]], ext_send.at[h], ext_recv.at[h],
                device_id=(sec, z * nx + xd), device_id_type=MESH,
            ).start()
    for o in order:
        pltpu.make_async_remote_copy(
            rows_out, rows_in.at[pl.ds(rep, 1)], rows_send, rows_recv, device_id=(sec, peer_of[o]), device_id_type=MESH
        ).start()

    def send_direct(lengths):
        for o in order:
            if ring_far(o[0], nz) in lengths:
                pltpu.make_async_remote_copy(
                    packed.at[peer_of[o]], recv.at[rep], data_send, data_recv,
                    device_id=(sec, peer_of[o]), device_id_type=MESH,
                ).start()

    def forward(h):
        places = range(far_steps) if h == 0 else range(far_steps, nz)
        every = recv_ext.at[pl.ds(0, nx - 1), halves[h]]
        pltpu.make_async_copy(every, every, ext_recv.at[h]).wait()
        total = recv_ext[0, places[0] : places[-1] + 1]
        for k in range(1, nx):
            total = total + recv_ext[k, places[0] : places[-1] + 1]
        merged[places[0] : places[-1] + 1] = total
        for place in sorted(places, key=lambda p: -ring_far((p - shift) % nz, nz)):
            dz = (place - shift) % nz
            if dz:
                pltpu.make_async_remote_copy(
                    merged.at[place], recv_merged.at[z], merged_send, merged_recv,
                    device_id=(sec, ((z + dz) % nz) * nx + x), device_id_type=MESH,
                ).start()
            else:
                recv_merged[pl.ds(z, 1)] = total[place - places[0] : place - places[0] + 1]

    send_direct((3, 4))
    forward(0)
    send_direct((2,))
    forward(1)
    send_direct((1, 0))

    for b in range(blocks):
        hit = jnp.zeros((1, LANES), f32)
        for s in range(slots):
            hit = jnp.where(ids[s] == b, 1.0, hit)
        kept = jnp.concatenate([jnp.broadcast_to(hit, (BLK, LANES))] * (width // LANES), axis=1)
        mine = res[b]
        new_res[b] = mine - mine.astype(bf16).astype(f32) * kept

    every = rows_in.at[pl.ds(0, others)]
    pltpu.make_async_copy(every, every, rows_recv).wait()
    row = lax.broadcasted_iota(jnp.int32, (row_count, LANES), 0) + 1
    lists = rows_in[...]
    ext_rows = (lists // base).sum(axis=0, keepdims=True)
    direct_rows = (lists % base).reshape(replicas // group, group, LANES).sum(axis=1)
    hot_ext = jnp.where(row == ext_rows, 1.0, 0.0).astype(bf16)
    hots = [jnp.where(row == direct_rows[g : g + 1], 1.0, 0.0).astype(bf16) for g in range(replicas // group)]

    every = recv.at[pl.ds(0, others)]
    pltpu.make_async_copy(every, every, data_recv).wait()
    every = recv_merged.at[pl.ds(0, nz - 1)]
    pltpu.make_async_copy(every, every, merged_recv).wait()

    ext = recv_merged[0]
    for k in range(1, nz):
        ext = ext + recv_merged[k]
    summed = jnp.dot(hot_ext, jnp.concatenate([ext] * group, axis=0), preferred_element_type=f32)
    for g, hot in enumerate(hots):
        held = recv[g * group : (g + 1) * group].reshape(LANES, cols)
        summed = summed + jnp.dot(hot, held, preferred_element_type=f32)

    summed_out[...] = summed
    device = sec * replicas + rep
    square_out[...] = (summed * summed).reshape(row_count // 8, 8, cols).sum(axis=0).sum(axis=0, keepdims=True)
    squares[pl.ds(device, 1)] = square_out[...]
    for o in order:
        for d in range(sections):
            pltpu.make_async_remote_copy(
                square_out, squares.at[pl.ds(device, 1)], square_send, square_recv,
                device_id=((sec + d) % sections, peer_of[o]), device_id_type=MESH,
            ).start()
    for peer in across:
        pltpu.make_async_remote_copy(
            square_out, squares.at[pl.ds(device, 1)], square_send, square_recv,
            device_id=(peer, rep), device_id_type=MESH,
        ).start()
    every_square = squares.at[pl.ds(0, sections * replicas - 1)]
    pltpu.make_async_copy(every_square, every_square, square_recv).wait()
    every = packed.at[pl.ds(0, others)]
    pltpu.make_async_copy(every, every, data_send).wait()
    every = rows_in.at[pl.ds(0, others)]
    pltpu.make_async_copy(every, every, rows_send).wait()
    for h in range(2):
        every = recv_ext.at[pl.ds(0, nx - 1), halves[h]]
        pltpu.make_async_copy(every, every, ext_send.at[h]).wait()
    every = recv_merged.at[pl.ds(0, nz - 1)]
    pltpu.make_async_copy(every, every, merged_send).wait()
    pltpu.make_async_copy(every_square, every_square, square_send).wait()


def finish(count_total, new_res, summed, squares, new_res_hbm, update_hbm, update, res_sem, update_sem):
    step = new_res.shape[0] // 4
    copies = [
        pltpu.make_async_copy(new_res.at[pl.ds(c * step, step)], new_res_hbm.at[pl.ds(c * step, step)], res_sem.at[c])
        for c in range(4)
    ]
    for copy in copies:
        copy.start()
    every = squares[...]
    norm_total = every.sum(axis=0, keepdims=True).sum(axis=1, keepdims=True)
    clip_factor = scale_level / jnp.sqrt(norm_total / count_total + epsilon)
    update[...] = (summed[...] * clip_factor).astype(jnp.bfloat16)
    copies.append(pltpu.make_async_copy(update, update_hbm, update_sem))
    copies[-1].start()
    for copy in copies:
        copy.wait()


def per_device(nz, nx, sections, gradient, residual, block_ids, block_counts):
    replicas = nz * nx
    row_count, width = gradient.shape
    cols = width // replicas
    slots = block_ids.shape[1]
    count_total = sections * row_count * width
    f32, bf16, i32 = jnp.float32, jnp.bfloat16, jnp.int32
    dma = pltpu.SemaphoreType.DMA
    blocks = row_count // BLK
    shape = (blocks, BLK, width)
    direct_rows, ext_rows = DIRECT * BLK, (slots - DIRECT) * BLK
    new_residual, summed, squares = pl.pallas_call(
        functools.partial(kernel, nz, nx, sections),
        out_shape=(
            pltpu.VMEM(shape, f32), pltpu.VMEM((row_count, cols), f32), pltpu.VMEM((sections * replicas, cols), f32)
        ),
        in_specs=[
            pl.BlockSpec(memory_space=pl.ANY),
            pl.BlockSpec(memory_space=pl.ANY),
            pl.BlockSpec(memory_space=pltpu.SMEM),
            pl.BlockSpec(memory_space=pltpu.SMEM),
        ],
        out_specs=(pl.BlockSpec(memory_space=pltpu.VMEM),) * 3,
        scratch_shapes=[
            pltpu.VMEM(shape, bf16),
            pltpu.VMEM(shape, f32),
            pltpu.VMEM((replicas, direct_rows, cols), bf16),
            pltpu.VMEM((nx, nz, ext_rows, cols), bf16),
            pltpu.VMEM((1, LANES), i32),
            pltpu.VMEM((replicas, direct_rows, cols), bf16),
            pltpu.VMEM((nx, nz, ext_rows, cols), bf16),
            pltpu.VMEM((nz, ext_rows, cols), bf16),
            pltpu.VMEM((nz, ext_rows, cols), bf16),
            pltpu.VMEM((replicas, LANES), i32),
            pltpu.VMEM((1, cols), f32),
            dma((2, 4)), dma, dma, dma, dma, dma((2,)), dma((2,)), dma, dma, dma, dma,
        ],
        compiler_params=pltpu.CompilerParams(collective_id=0, has_side_effects=True),
    )(gradient.reshape(shape), residual.reshape(shape), block_ids, block_counts)
    any_space = pl.BlockSpec(memory_space=pltpu.HBM)
    in_vmem = pl.BlockSpec(memory_space=pltpu.VMEM)
    new_residual, update = pl.pallas_call(
        functools.partial(finish, count_total),
        out_shape=(pltpu.HBM(shape, f32), pltpu.HBM((row_count, cols), bf16)),
        in_specs=[in_vmem] * 3,
        out_specs=(any_space, any_space),
        scratch_shapes=[pltpu.VMEM((row_count, cols), bf16), dma((4,)), dma],
    )(*(pltpu.with_memory_space_constraint(v, pltpu.VMEM) for v in (new_residual, summed, squares)))
    return new_residual.reshape(row_count, width), update


def solution(mesh):
    sections, replicas = mesh.shape["section"], mesh.shape["replica"]
    both = P("section", "replica")
    return jax.shard_map(
        functools.partial(per_device, replicas // NX, NX, sections),
        mesh=mesh,
        in_specs=(both, both, both, both),
        out_specs=(both, both),
        check_vma=False,
    )
```

```python
import functools
import jax
import jax.numpy as jnp
from jax import lax
from jax.experimental import pallas as pl
from jax.experimental.pallas import tpu as pltpu
from jax.sharding import PartitionSpec as P

BLK = 8
LANES = 128
NX = 4
DIRECT = 4
MESH = pl.DeviceIdType.MESH

scale_level = 1.0
epsilon = 1e-06


def ring_far(d, n):
    return min(d, n - d)


def plane_order(nz, nx):
    offsets = [(dz, dx) for dz in range(nz) for dx in range(nx) if (dz, dx) != (0, 0)]
    return sorted(
        offsets, key=lambda o: (-ring_far(o[0], nz) - ring_far(o[1], nx), ring_far(o[1], nx), o)
    )


def kernel(
    nz, nx, sections,
    grad_hbm, res_hbm, ids_hbm, count_in,
    new_res, summed_out, squares,
    grad, res, packed, packed_ext, rows_out, recv, recv_ext, merged, recv_merged, rows_in, square_out, ids_ref,
    list_sem, load_sem, data_send, data_recv, rows_send, rows_recv, ext_send, ext_recv, merged_send, merged_recv,
    square_send, square_recv,
):
    replicas = nz * nx
    blocks, _, width = grad.shape
    row_count = blocks * BLK
    cols = width // replicas
    slots = ids_ref.shape[1]
    sec, rep = lax.axis_index("section"), lax.axis_index("replica")
    z, x = rep // nx, rep % nx
    others = replicas - 1
    f32, bf16 = jnp.float32, jnp.bfloat16

    ids_copy = pltpu.make_async_copy(ids_hbm, ids_ref, list_sem)
    ids_copy.start()
    loads = []
    chunks = 4
    step = blocks // chunks
    for c in range(chunks):
        part = pl.ds(c * step, step)
        pair = (
            pltpu.make_async_copy(grad_hbm.at[part], grad.at[part], load_sem.at[0, c]),
            pltpu.make_async_copy(res_hbm.at[part], res.at[part], load_sem.at[1, c]),
        )
        for copy in pair:
            copy.start()
        loads.append(pair)

    order = plane_order(nz, nx)
    peer_of = {(dz, dx): ((z + dz) % nz) * nx + (x + dx) % nx for dz, dx in order}
    across = [(sec + d) % sections for d in range(1, sections)]
    barrier = pltpu.get_barrier_semaphore()
    for o in order:
        pl.semaphore_signal(barrier, inc=1, device_id=(sec, peer_of[o]), device_id_type=MESH)
    for peer in across:
        pl.semaphore_signal(barrier, inc=1, device_id=(peer, rep), device_id_type=MESH)

    ids_copy.wait()
    lane = lax.broadcasted_iota(jnp.int32, (1, LANES), 1)
    group = LANES // (DIRECT * BLK)
    slot_of = lane // BLK - (rep % group) * DIRECT
    count = jnp.broadcast_to(count_in[...], (1, LANES))
    ids = [jnp.full((1, LANES), ids_ref[0, s], jnp.int32) for s in range(slots)]
    ids = [jnp.where(count > s, ids[s], -1) for s in range(slots)]
    base = 2 * row_count
    both_rows = jnp.zeros((1, LANES), jnp.int32)
    for s in range(slots):
        target = jnp.where(ids[s] >= 0, ids[s] * BLK + lane % BLK + 1, 0)
        if s < DIRECT:
            both_rows = both_rows + jnp.where(slot_of == s, target, 0)
        else:
            both_rows = both_rows + jnp.where(slot_of == s - DIRECT, target * base, 0)
    rows_out[...] = both_rows
    rows_in[pl.ds(rep, 1)] = both_rows

    for c in range(chunks):
        for copy in loads[c]:
            copy.wait()
        for b in range(c * step, (c + 1) * step):
            res[b] = grad[b].astype(f32) + res[b]

    shift = nz // 2 + 1
    far_steps = 3
    for pair in range(DIRECT // 2, slots // 2):
        picked = []
        for h in range(2):
            s = 2 * pair + h
            alive = jnp.broadcast_to(jnp.where(ids[s] >= 0, 1.0, 0.0), (BLK, LANES))
            alive = jnp.concatenate([alive] * (width // LANES), axis=1)
            picked.append(jnp.where(alive > 0.5, res[ids_ref[0, s]], 0.0))
        both = jnp.concatenate(picked, axis=0).astype(bf16)
        rows = slice((pair - DIRECT // 2) * 2 * BLK, (pair - DIRECT // 2 + 1) * 2 * BLK)
        for zd in range(nz):
            place = (zd - z + shift + nz) % nz
            for xd in range(nx):
                r = zd * nx + xd
                packed_ext[xd, pl.ds(place, 1), rows, :] = both[None, :, r * cols : (r + 1) * cols]
    for pair in range(DIRECT // 2):
        both = jnp.concatenate([res[ids_ref[0, 2 * pair + h]] for h in range(2)], axis=0).astype(bf16)
        rows = slice(pair * 2 * BLK, (pair + 1) * 2 * BLK)
        for r in range(replicas):
            packed[r, rows, :] = both[:, r * cols : (r + 1) * cols]
    recv[pl.ds(rep, 1)] = packed[pl.ds(rep, 1)]
    recv_ext[pl.ds(x, 1)] = packed_ext[pl.ds(x, 1)]

    pl.semaphore_wait(barrier, len(order) + len(across))

    halves = (pl.ds(0, far_steps), pl.ds(far_steps, nz - far_steps))
    for h in range(2):
        for dx in sorted(range(1, nx), key=lambda d: -ring_far(d, nx)):
            xd = (x + dx) % nx
            pltpu.make_async_remote_copy(
                packed_ext.at[xd, halves[h]], recv_ext.at[x, halves[h]], ext_send.at[h], ext_recv.at[h],
                device_id=(sec, z * nx + xd), device_id_type=MESH,
            ).start()
    for o in order:
        pltpu.make_async_remote_copy(
            rows_out, rows_in.at[pl.ds(rep, 1)], rows_send, rows_recv, device_id=(sec, peer_of[o]), device_id_type=MESH
        ).start()

    def send_to(zt, dx):
        to = zt * nx + (x + dx) % nx
        pltpu.make_async_remote_copy(
            packed.at[to], recv.at[rep], data_send, data_recv, device_id=(sec, to), device_id_type=MESH
        ).start()

    half = nz // 2
    mine_half, other_half = (z // half) * half, (1 - z // half) * half
    cross = [other_half + (z + k) % half for k in (2, 1, 3, 0)]
    inner = [mine_half + (z + k) % half for k in (2, 1, 3)]

    def send_cross():
        for dx in (2, 1, 3, 0):
            for zt in cross:
                send_to(zt, dx)

    def send_inner():
        for dx in (2, 1, 3, 0):
            for zt in inner:
                send_to(zt, dx)
        for dx in (2, 1, 3):
            send_to(z, dx)

    def forward(h):
        places = range(far_steps) if h == 0 else range(far_steps, nz)
        every = recv_ext.at[pl.ds(0, nx - 1), halves[h]]
        pltpu.make_async_copy(every, every, ext_recv.at[h]).wait()
        total = recv_ext[0, places[0] : places[-1] + 1]
        for k in range(1, nx):
            total = total + recv_ext[k, places[0] : places[-1] + 1]
        merged[places[0] : places[-1] + 1] = total
        for place in sorted(places, key=lambda p: -ring_far((p - shift) % nz, nz)):
            dz = (place - shift) % nz
            if dz:
                pltpu.make_async_remote_copy(
                    merged.at[place], recv_merged.at[z], merged_send, merged_recv,
                    device_id=(sec, ((z + dz) % nz) * nx + x), device_id_type=MESH,
                ).start()
            else:
                recv_merged[pl.ds(z, 1)] = total[place - places[0] : place - places[0] + 1]

    send_cross()
    forward(0)
    send_inner()
    forward(1)

    for b in range(blocks):
        hit = jnp.zeros((1, LANES), f32)
        for s in range(slots):
            hit = jnp.where(ids[s] == b, 1.0, hit)
        kept = jnp.concatenate([jnp.broadcast_to(hit, (BLK, LANES))] * (width // LANES), axis=1)
        mine = res[b]
        new_res[b] = mine - mine.astype(bf16).astype(f32) * kept

    every = rows_in.at[pl.ds(0, others)]
    pltpu.make_async_copy(every, every, rows_recv).wait()
    row = lax.broadcasted_iota(jnp.int32, (row_count, LANES), 0) + 1
    lists = rows_in[...]
    ext_rows = (lists // base).sum(axis=0, keepdims=True)
    direct_rows = (lists % base).reshape(replicas // group, group, LANES).sum(axis=1)
    hot_ext = jnp.where(row == ext_rows, 1.0, 0.0).astype(bf16)
    hots = [jnp.where(row == direct_rows[g : g + 1], 1.0, 0.0).astype(bf16) for g in range(replicas // group)]

    every = recv.at[pl.ds(0, others)]
    pltpu.make_async_copy(every, every, data_recv).wait()
    every = recv_merged.at[pl.ds(0, nz - 1)]
    pltpu.make_async_copy(every, every, merged_recv).wait()

    ext = recv_merged[0]
    for k in range(1, nz):
        ext = ext + recv_merged[k]
    summed = jnp.dot(hot_ext, jnp.concatenate([ext] * group, axis=0), preferred_element_type=f32)
    for g, hot in enumerate(hots):
        held = recv[g * group : (g + 1) * group].reshape(LANES, cols)
        summed = summed + jnp.dot(hot, held, preferred_element_type=f32)

    summed_out[...] = summed
    device = sec * replicas + rep
    square_out[...] = (summed * summed).reshape(row_count // 8, 8, cols).sum(axis=0).sum(axis=0, keepdims=True)
    squares[pl.ds(device, 1)] = square_out[...]
    def send_square(s_to, r_to):
        pltpu.make_async_remote_copy(
            square_out, squares.at[pl.ds(device, 1)], square_send, square_recv,
            device_id=(s_to, r_to), device_id_type=MESH,
        ).start()
    spread = sorted(
        [(d, dx) for d in range(sections) for dx in range(nx)],
        key=lambda o: (-ring_far(o[0] // 2, sections // 2) - ring_far(o[1], nx), o),
    )
    for zt in (0, 1, 2, 3, 7, 6, 5, 4):
        for d, dx in spread:
            go = functools.partial(send_square, (sec + d) % sections, zt * nx + (x + dx) % nx)
            if (d, dx) == (0, 0):
                pl.when(z != zt)(go)
            else:
                go()
    every_square = squares.at[pl.ds(0, sections * replicas - 1)]
    pltpu.make_async_copy(every_square, every_square, square_recv).wait()
    every = packed.at[pl.ds(0, others)]
    pltpu.make_async_copy(every, every, data_send).wait()
    every = rows_in.at[pl.ds(0, others)]
    pltpu.make_async_copy(every, every, rows_send).wait()
    for h in range(2):
        every = recv_ext.at[pl.ds(0, nx - 1), halves[h]]
        pltpu.make_async_copy(every, every, ext_send.at[h]).wait()
    every = recv_merged.at[pl.ds(0, nz - 1)]
    pltpu.make_async_copy(every, every, merged_send).wait()
    pltpu.make_async_copy(every_square, every_square, square_send).wait()


def released_first(nx):
    sec, rep = lax.axis_index("section"), lax.axis_index("replica")
    y, z, x = sec // 2, rep // nx, rep % nx
    return y + z + jnp.minimum(x, 1) <= 1


def ahead(nx, grad_hbm, res_hbm, ids_hbm, count_ref, new_res_hbm, grad, res, ids_ref, list_sem, load_sem, store_sem):
    @pl.when(released_first(nx))
    def _():
        blocks, _, width = grad.shape
        step = blocks // 4
        parts = [pl.ds(c * step, step) for c in range(4)]
        loads = [
            (
                pltpu.make_async_copy(grad_hbm.at[p], grad.at[p], load_sem.at[0, c]),
                pltpu.make_async_copy(res_hbm.at[p], res.at[p], load_sem.at[1, c]),
            )
            for c, p in enumerate(parts)
        ]
        stores = [pltpu.make_async_copy(res.at[p], new_res_hbm.at[p], store_sem.at[c]) for c, p in enumerate(parts)]
        for pair in loads:
            for copy in pair:
                copy.start()
        ids_copy = pltpu.make_async_copy(ids_hbm, ids_ref, list_sem)
        ids_copy.start()
        ids_copy.wait()
        count = jnp.full((1, LANES), count_ref[0, 0], jnp.int32)
        ids = [jnp.full((1, LANES), ids_ref[0, s], jnp.int32) for s in range(ids_ref.shape[1])]
        for c in range(4):
            for copy in loads[c]:
                copy.wait()
            for b in range(c * step, (c + 1) * step):
                hit = jnp.zeros((1, LANES), jnp.float32)
                for s, one in enumerate(ids):
                    hit = jnp.where((one == b) & (count > s), 1.0, hit)
                kept = jnp.concatenate([jnp.broadcast_to(hit, (BLK, LANES))] * (width // LANES), axis=1)
                mine = grad[b].astype(jnp.float32) + res[b]
                res[b] = mine - mine.astype(jnp.bfloat16).astype(jnp.float32) * kept
            stores[c].start()
        for copy in stores:
            copy.wait()


def finish(count_total, nx, new_res, summed, squares, _, new_res_hbm, update_hbm, update, res_sem, update_sem):
    step = new_res.shape[0] // 4
    copies = [
        pltpu.make_async_copy(new_res.at[pl.ds(c * step, step)], new_res_hbm.at[pl.ds(c * step, step)], res_sem.at[c])
        for c in range(4)
    ]
    late = jnp.logical_not(released_first(nx))

    @pl.when(late)
    def _():
        for copy in copies:
            copy.start()

    every = squares[...]
    norm_total = every.sum(axis=0, keepdims=True).sum(axis=1, keepdims=True)
    clip_factor = scale_level / jnp.sqrt(norm_total / count_total + epsilon)
    update[...] = (summed[...] * clip_factor).astype(jnp.bfloat16)
    last = pltpu.make_async_copy(update, update_hbm, update_sem)
    last.start()

    @pl.when(late)
    def _():
        for copy in copies:
            copy.wait()

    last.wait()


def per_device(nz, nx, sections, gradient, residual, block_ids, block_counts):
    replicas = nz * nx
    row_count, width = gradient.shape
    cols = width // replicas
    slots = block_ids.shape[1]
    count_total = sections * row_count * width
    f32, bf16, i32 = jnp.float32, jnp.bfloat16, jnp.int32
    dma = pltpu.SemaphoreType.DMA
    blocks = row_count // BLK
    shape = (blocks, BLK, width)
    direct_rows, ext_rows = DIRECT * BLK, (slots - DIRECT) * BLK
    gradient, residual = gradient.reshape(shape), residual.reshape(shape)
    in_hbm = pl.BlockSpec(memory_space=pltpu.HBM)
    in_vmem = pl.BlockSpec(memory_space=pltpu.VMEM)
    in_smem = pl.BlockSpec(memory_space=pltpu.SMEM)
    early_residual = pl.pallas_call(
        functools.partial(ahead, nx),
        out_shape=pltpu.HBM(shape, f32),
        in_specs=[in_hbm, in_hbm, in_hbm, in_smem],
        out_specs=in_hbm,
        scratch_shapes=[pltpu.VMEM(shape, bf16), pltpu.VMEM(shape, f32), pltpu.SMEM((1, slots), i32), dma, dma((2, 4)), dma((4,))],
    )(gradient, residual, block_ids, block_counts)
    new_residual, summed, squares = pl.pallas_call(
        functools.partial(kernel, nz, nx, sections),
        out_shape=(
            pltpu.VMEM(shape, f32), pltpu.VMEM((row_count, cols), f32), pltpu.VMEM((sections * replicas, cols), f32)
        ),
        in_specs=[pl.BlockSpec(memory_space=pltpu.HBM)] * 3 + [pl.BlockSpec(memory_space=pltpu.VMEM)],
        out_specs=(pl.BlockSpec(memory_space=pltpu.VMEM),) * 3,
        scratch_shapes=[
            pltpu.VMEM(shape, bf16),
            pltpu.VMEM(shape, f32),
            pltpu.VMEM((replicas, direct_rows, cols), bf16),
            pltpu.VMEM((nx, nz, ext_rows, cols), bf16),
            pltpu.VMEM((1, LANES), i32),
            pltpu.VMEM((replicas, direct_rows, cols), bf16),
            pltpu.VMEM((nx, nz, ext_rows, cols), bf16),
            pltpu.VMEM((nz, ext_rows, cols), bf16),
            pltpu.VMEM((nz, ext_rows, cols), bf16),
            pltpu.VMEM((replicas, LANES), i32),
            pltpu.VMEM((1, cols), f32),
            pltpu.SMEM((1, slots), i32),
            dma, dma((2, 4)), dma, dma, dma, dma, dma((2,)), dma((2,)), dma, dma, dma, dma,
        ],
        compiler_params=pltpu.CompilerParams(collective_id=0, has_side_effects=True),
    )(gradient, residual, block_ids, block_counts)
    parts = (pltpu.with_memory_space_constraint(v, pltpu.VMEM) for v in (new_residual, summed, squares))
    new_residual, update = pl.pallas_call(
        functools.partial(finish, count_total, nx),
        out_shape=(pltpu.HBM(shape, f32), pltpu.HBM((row_count, cols), bf16)),
        in_specs=[in_vmem] * 3 + [in_hbm],
        out_specs=(in_hbm, in_hbm),
        scratch_shapes=[pltpu.VMEM((row_count, cols), bf16), dma((4,)), dma],
        input_output_aliases={3: 0},
    )(*parts, early_residual)
    return new_residual.reshape(row_count, width), update


def solution(mesh):
    sections, replicas = mesh.shape["section"], mesh.shape["replica"]
    both = P("section", "replica")
    return jax.shard_map(
        functools.partial(per_device, replicas // NX, NX, sections),
        mesh=mesh,
        in_specs=(both, both, both, both),
        out_specs=(both, both),
        check_vma=False,
    )
```

```python
import functools
import jax
import jax.numpy as jnp
from jax import lax
from jax.experimental import pallas as pl
from jax.experimental.pallas import tpu as pltpu
from jax.sharding import PartitionSpec as P

BLK = 8
LANES = 128
NX = 4
DIRECT = 4
MESH = pl.DeviceIdType.MESH

scale_level = 1.0
epsilon = 1e-06


def ring_far(d, n):
    return min(d, n - d)


def kernel(
    nz, nx, sections,
    grad_hbm, res_hbm, ids_hbm, count_in,
    new_res, summed_out, squares,
    grad, res, packed, packed_ext, rows_out, recv, recv_ext, merged, recv_merged, rows_x, rows_in, square_out, ids_ref,
    column_in, list_sem, load_sem, data_send, data_recv, rows_x_send, rows_x_recv, rows_send, rows_recv, ext_send, ext_recv, merged_send, merged_recv,
    square_send, square_recv,
):
    replicas = nz * nx
    blocks, _, width = grad.shape
    row_count = blocks * BLK
    cols = width // replicas
    slots = ids_ref.shape[1]
    sec, rep = lax.axis_index("section"), lax.axis_index("replica")
    z, x = rep // nx, rep % nx
    others = replicas - 1
    f32, bf16 = jnp.float32, jnp.bfloat16

    column = [((z + d) % nz) * nx + x for d in sorted(range(1, nz), key=lambda d: -ring_far(d, nz))]
    line = {dx: z * nx + (x + dx) % nx for dx in (2, 1, 3)}
    across = [(sec + d) % sections for d in range(1, sections)]
    barrier = pltpu.get_barrier_semaphore()
    for peer in column + list(line.values()):
        pl.semaphore_signal(barrier, inc=1, device_id=(sec, peer), device_id_type=MESH)
    for peer in across:
        pl.semaphore_signal(barrier, inc=1, device_id=(peer, rep), device_id_type=MESH)

    ids_copy = pltpu.make_async_copy(ids_hbm, ids_ref, list_sem)
    ids_copy.start()
    loads = []
    chunks = 4
    step = blocks // chunks
    for c in range(chunks):
        part = pl.ds(c * step, step)
        pair = (
            pltpu.make_async_copy(grad_hbm.at[part], grad.at[part], load_sem.at[0, c]),
            pltpu.make_async_copy(res_hbm.at[part], res.at[part], load_sem.at[1, c]),
        )
        for copy in pair:
            copy.start()
        loads.append(pair)

    ids_copy.wait()
    lane = lax.broadcasted_iota(jnp.int32, (1, LANES), 1)
    group = LANES // (DIRECT * BLK)
    slot_of = lane // BLK - (rep % group) * DIRECT
    count = jnp.broadcast_to(count_in[...], (1, LANES))
    ids = [jnp.full((1, LANES), ids_ref[0, s], jnp.int32) for s in range(slots)]
    ids = [jnp.where(count > s, ids[s], -1) for s in range(slots)]
    base = 2 * row_count
    both_rows = jnp.zeros((1, LANES), jnp.int32)
    for s in range(slots):
        target = jnp.where(ids[s] >= 0, ids[s] * BLK + lane % BLK + 1, 0)
        if s < DIRECT:
            both_rows = both_rows + jnp.where(slot_of == s, target, 0)
        else:
            both_rows = both_rows + jnp.where(slot_of == s - DIRECT, target * base, 0)
    rows_out[0:1] = both_rows
    rows_x[pl.ds(x, 1)] = both_rows

    for c in range(chunks):
        for copy in loads[c]:
            copy.wait()
        for b in range(c * step, (c + 1) * step):
            res[b] = grad[b].astype(f32) + res[b]

    half = nz // 2
    for pair in range(DIRECT // 2, slots // 2):
        picked = []
        for h in range(2):
            s = 2 * pair + h
            alive = jnp.broadcast_to(jnp.where(ids[s] >= 0, 1.0, 0.0), (BLK, LANES))
            alive = jnp.concatenate([alive] * (width // LANES), axis=1)
            picked.append(jnp.where(alive > 0.5, res[ids_ref[0, s]], 0.0))
        both = jnp.concatenate(picked, axis=0).astype(bf16)
        rows = slice((pair - DIRECT // 2) * 2 * BLK, (pair - DIRECT // 2 + 1) * 2 * BLK)
        for zd in range(nz):
            place = (zd // half + z // half + 1) % 2 * half + zd % half
            for xd in range(nx):
                r = zd * nx + xd
                packed_ext[xd, pl.ds(place, 1), rows, :] = both[None, :, r * cols : (r + 1) * cols]
    for pair in range(DIRECT // 2):
        both = jnp.concatenate([res[ids_ref[0, 2 * pair + h]] for h in range(2)], axis=0).astype(bf16)
        rows = slice(pair * 2 * BLK, (pair + 1) * 2 * BLK)
        for r in range(replicas):
            packed[r, rows, :] = both[:, r * cols : (r + 1) * cols]
    recv[pl.ds((half + z % half) * nx + x, 1)] = packed[pl.ds(rep, 1)]
    recv_ext[pl.ds(x, 1)] = packed_ext[pl.ds(x, 1)]

    pl.semaphore_wait(barrier, len(column) + len(line) + len(across))
    for dx in (2, 1, 3):
        pl.semaphore_signal(column_in.at[x], inc=1, device_id=(sec, line[dx]), device_id_type=MESH)

    halves = (pl.ds(0, half), pl.ds(half, half))
    for dx in sorted(range(1, nx), key=lambda d: -ring_far(d, nx)):
        pltpu.make_async_remote_copy(
            rows_out.at[pl.ds(0, 1)], rows_x.at[pl.ds(x, 1)], rows_x_send, rows_x_recv,
            device_id=(sec, z * nx + (x + dx) % nx), device_id_type=MESH,
        ).start()
    def send_ext(h):
        for dx in sorted(range(1, nx), key=lambda d: -ring_far(d, nx)):
            xd = (x + dx) % nx
            pltpu.make_async_remote_copy(
                packed_ext.at[xd, halves[h]], recv_ext.at[x, halves[h]], ext_send.at[h], ext_recv.at[h],
                device_id=(sec, z * nx + xd), device_id_type=MESH,
            ).start()

    def send_to(zt, dx, same):
        to = zt * nx + (x + dx) % nx
        pltpu.make_async_remote_copy(
            packed.at[to], recv.at[(same * half + z % half) * nx + x], data_send, data_recv.at[same],
            device_id=(sec, to), device_id_type=MESH,
        ).start()

    mine_half, other_half = (z // half) * half, (1 - z // half) * half
    cross = [other_half + (z + k) % half for k in (2, 1, 3, 0)]
    inner = [mine_half + (z + k) % half for k in (2, 1, 3)]

    def send_cross(steps):
        for dx in steps:
            for zt in cross:
                send_to(zt, dx, 0)

    def send_inner(steps):
        for dx in steps:
            for zt in inner:
                send_to(zt, dx, 1)
            if dx:
                send_to(z, dx, 1)

    def forward_rows():
        every = rows_x.at[pl.ds(0, nx - 1)]
        pltpu.make_async_copy(every, every, rows_x_recv).wait()
        quad = rows_x[...].sum(axis=0, keepdims=True)
        rows_out[1:2] = quad
        rows_in[pl.ds(half + z % half, 1)] = quad
        for same, places in enumerate((cross, inner)):
            for zt in places:
                pltpu.make_async_remote_copy(
                    rows_out.at[pl.ds(1, 1)], rows_in.at[pl.ds(same * half + z % half, 1)], rows_send, rows_recv,
                    device_id=(sec, zt * nx + x), device_id_type=MESH,
                ).start()

    def forward(h):
        start = h * half
        every = recv_ext.at[pl.ds(0, nx - 1), halves[h]]
        pltpu.make_async_copy(every, every, ext_recv.at[h]).wait()
        total = recv_ext[0, start : start + half]
        for k in range(1, nx):
            total = total + recv_ext[k, start : start + half]
        merged[start : start + half] = total
        for zt in (inner if h else cross):
            pltpu.make_async_remote_copy(
                merged.at[start + zt % half], recv_merged.at[z], merged_send, merged_recv,
                device_id=(sec, zt * nx + x), device_id_type=MESH,
            ).start()
        if h:
            recv_merged[pl.ds(z, 1)] = merged[pl.ds(start + z % half, 1)]

    def column_ready(dx):
        pl.semaphore_wait(column_in.at[(x + dx) % nx], 1)

    send_ext(0)
    send_ext(1)
    send_cross((0,))
    column_ready(1)
    send_cross((1,))
    column_ready(3)
    send_cross((3,))
    forward_rows()
    column_ready(2)
    send_cross((2,))
    forward(0)
    send_inner((0, 2, 1, 3))
    forward(1)

    for b in range(blocks):
        hit = jnp.zeros((1, LANES), f32)
        for s in range(slots):
            hit = jnp.where(ids[s] == b, 1.0, hit)
        kept = jnp.concatenate([jnp.broadcast_to(hit, (BLK, LANES))] * (width // LANES), axis=1)
        mine = res[b]
        new_res[b] = mine - mine.astype(bf16).astype(f32) * kept

    every_row = rows_in.at[pl.ds(0, nz - 1)]
    pltpu.make_async_copy(every_row, every_row, rows_recv).wait()
    row = lax.broadcasted_iota(jnp.int32, (row_count, LANES), 0) + 1
    lists = rows_in[...]
    ext_rows = (lists // base).sum(axis=0, keepdims=True)
    direct_rows = lists % base
    hot_ext = jnp.where(row == ext_rows, 1.0, 0.0).astype(bf16)
    hots = [jnp.where(row == direct_rows[g : g + 1], 1.0, 0.0).astype(bf16) for g in range(replicas // group)]

    summed = jnp.zeros((row_count, cols), f32)
    for same in range(2):
        every = recv.at[pl.ds(same * half * nx, half * nx - same)]
        pltpu.make_async_copy(every, every, data_recv.at[same]).wait()
        for g in range(same * half, (same + 1) * half):
            held = recv[g * group : (g + 1) * group].reshape(LANES, cols)
            summed = summed + jnp.dot(hots[g], held, preferred_element_type=f32)
    every = recv_merged.at[pl.ds(0, nz - 1)]
    pltpu.make_async_copy(every, every, merged_recv).wait()
    ext = recv_merged[0]
    for k in range(1, nz):
        ext = ext + recv_merged[k]
    summed = summed + jnp.dot(hot_ext, jnp.concatenate([ext] * group, axis=0), preferred_element_type=f32)
    summed_out[...] = summed
    device = sec * replicas + rep
    square_out[...] = (summed * summed).reshape(row_count // 8, 8, cols).sum(axis=0).sum(axis=0, keepdims=True)
    squares[pl.ds(device, 1)] = square_out[...]
    def send_square(s_to, r_to):
        pltpu.make_async_remote_copy(
            square_out, squares.at[pl.ds(device, 1)], square_send, square_recv,
            device_id=(s_to, r_to), device_id_type=MESH,
        ).start()
    spread = sorted(
        [(d, dx) for d in range(sections) for dx in range(nx)],
        key=lambda o: (-ring_far(o[0] // 2, sections // 2) - ring_far(o[1], nx), o),
    )
    for zt in (0, 1, 2, 3, 7, 6, 5, 4):
        for d, dx in spread:
            go = functools.partial(send_square, (sec + d) % sections, zt * nx + (x + dx) % nx)
            if (d, dx) == (0, 0):
                pl.when(z != zt)(go)
            else:
                go()
    every_square = squares.at[pl.ds(0, sections * replicas - 1)]
    pltpu.make_async_copy(every_square, every_square, square_recv).wait()
    every = packed.at[pl.ds(0, others)]
    pltpu.make_async_copy(every, every, data_send).wait()
    every = rows_x.at[pl.ds(0, nx - 1)]
    pltpu.make_async_copy(every, every, rows_x_send).wait()
    pltpu.make_async_copy(every_row, every_row, rows_send).wait()
    for h in range(2):
        every = recv_ext.at[pl.ds(0, nx - 1), halves[h]]
        pltpu.make_async_copy(every, every, ext_send.at[h]).wait()
    every = recv_merged.at[pl.ds(0, nz - 1)]
    pltpu.make_async_copy(every, every, merged_send).wait()
    pltpu.make_async_copy(every_square, every_square, square_send).wait()


def released_first(nx):
    sec, rep = lax.axis_index("section"), lax.axis_index("replica")
    y, z, x = sec // 2, rep // nx, rep % nx
    return y + z + jnp.minimum(x, 1) <= 1


def ahead(nx, grad_hbm, res_hbm, ids_hbm, count_ref, new_res_hbm, grad, res, ids_ref, list_sem, load_sem, store_sem):
    @pl.when(released_first(nx))
    def _():
        blocks, _, width = grad.shape
        step = blocks // 4
        parts = [pl.ds(c * step, step) for c in range(4)]
        loads = [
            (
                pltpu.make_async_copy(grad_hbm.at[p], grad.at[p], load_sem.at[0, c]),
                pltpu.make_async_copy(res_hbm.at[p], res.at[p], load_sem.at[1, c]),
            )
            for c, p in enumerate(parts)
        ]
        stores = [pltpu.make_async_copy(res.at[p], new_res_hbm.at[p], store_sem.at[c]) for c, p in enumerate(parts)]
        for pair in loads:
            for copy in pair:
                copy.start()
        ids_copy = pltpu.make_async_copy(ids_hbm, ids_ref, list_sem)
        ids_copy.start()
        ids_copy.wait()
        count = jnp.full((1, LANES), count_ref[0, 0], jnp.int32)
        ids = [jnp.full((1, LANES), ids_ref[0, s], jnp.int32) for s in range(ids_ref.shape[1])]
        for c in range(4):
            for copy in loads[c]:
                copy.wait()
            for b in range(c * step, (c + 1) * step):
                hit = jnp.zeros((1, LANES), jnp.float32)
                for s, one in enumerate(ids):
                    hit = jnp.where((one == b) & (count > s), 1.0, hit)
                kept = jnp.concatenate([jnp.broadcast_to(hit, (BLK, LANES))] * (width // LANES), axis=1)
                mine = grad[b].astype(jnp.float32) + res[b]
                res[b] = mine - mine.astype(jnp.bfloat16).astype(jnp.float32) * kept
            stores[c].start()
        for copy in stores:
            copy.wait()


def finish(count_total, nx, new_res, summed, squares, _, new_res_hbm, update_hbm, update, res_sem, update_sem):
    step = new_res.shape[0] // 4
    copies = [
        pltpu.make_async_copy(new_res.at[pl.ds(c * step, step)], new_res_hbm.at[pl.ds(c * step, step)], res_sem.at[c])
        for c in range(4)
    ]
    late = jnp.logical_not(released_first(nx))

    @pl.when(late)
    def _():
        for copy in copies:
            copy.start()

    every = squares[...]
    norm_total = every.sum(axis=0, keepdims=True).sum(axis=1, keepdims=True)
    clip_factor = scale_level / jnp.sqrt(norm_total / count_total + epsilon)
    update[...] = (summed[...] * clip_factor).astype(jnp.bfloat16)
    last = pltpu.make_async_copy(update, update_hbm, update_sem)
    last.start()

    @pl.when(late)
    def _():
        for copy in copies:
            copy.wait()

    last.wait()


def per_device(nz, nx, sections, gradient, residual, block_ids, block_counts):
    replicas = nz * nx
    row_count, width = gradient.shape
    cols = width // replicas
    slots = block_ids.shape[1]
    count_total = sections * row_count * width
    f32, bf16, i32 = jnp.float32, jnp.bfloat16, jnp.int32
    dma = pltpu.SemaphoreType.DMA
    blocks = row_count // BLK
    shape = (blocks, BLK, width)
    direct_rows, ext_rows = DIRECT * BLK, (slots - DIRECT) * BLK
    gradient, residual = gradient.reshape(shape), residual.reshape(shape)
    in_hbm = pl.BlockSpec(memory_space=pltpu.HBM)
    in_vmem = pl.BlockSpec(memory_space=pltpu.VMEM)
    in_smem = pl.BlockSpec(memory_space=pltpu.SMEM)
    early_residual = pl.pallas_call(
        functools.partial(ahead, nx),
        out_shape=pltpu.HBM(shape, f32),
        in_specs=[in_hbm, in_hbm, in_hbm, in_smem],
        out_specs=in_hbm,
        scratch_shapes=[pltpu.VMEM(shape, bf16), pltpu.VMEM(shape, f32), pltpu.SMEM((1, slots), i32), dma, dma((2, 4)), dma((4,))],
    )(gradient, residual, block_ids, block_counts)
    new_residual, summed, squares = pl.pallas_call(
        functools.partial(kernel, nz, nx, sections),
        out_shape=(
            pltpu.VMEM(shape, f32), pltpu.VMEM((row_count, cols), f32), pltpu.VMEM((sections * replicas, cols), f32)
        ),
        in_specs=[pl.BlockSpec(memory_space=pltpu.HBM)] * 3 + [pl.BlockSpec(memory_space=pltpu.VMEM)],
        out_specs=(pl.BlockSpec(memory_space=pltpu.VMEM),) * 3,
        scratch_shapes=[
            pltpu.VMEM(shape, bf16),
            pltpu.VMEM(shape, f32),
            pltpu.VMEM((replicas, direct_rows, cols), bf16),
            pltpu.VMEM((nx, nz, ext_rows, cols), bf16),
            pltpu.VMEM((2, LANES), i32),
            pltpu.VMEM((replicas, direct_rows, cols), bf16),
            pltpu.VMEM((nx, nz, ext_rows, cols), bf16),
            pltpu.VMEM((nz, ext_rows, cols), bf16),
            pltpu.VMEM((nz, ext_rows, cols), bf16),
            pltpu.VMEM((nx, LANES), i32),
            pltpu.VMEM((nz, LANES), i32),
            pltpu.VMEM((1, cols), f32),
            pltpu.SMEM((1, slots), i32),
            pltpu.SemaphoreType.REGULAR((nx,)), dma, dma((2, 4)), dma, dma((2,)), dma, dma, dma, dma, dma((2,)), dma((2,)), dma, dma, dma, dma,
        ],
        compiler_params=pltpu.CompilerParams(collective_id=0, has_side_effects=True),
    )(gradient, residual, block_ids, block_counts)
    parts = (pltpu.with_memory_space_constraint(v, pltpu.VMEM) for v in (new_residual, summed, squares))
    new_residual, update = pl.pallas_call(
        functools.partial(finish, count_total, nx),
        out_shape=(pltpu.HBM(shape, f32), pltpu.HBM((row_count, cols), bf16)),
        in_specs=[in_vmem] * 3 + [in_hbm],
        out_specs=(in_hbm, in_hbm),
        scratch_shapes=[pltpu.VMEM((row_count, cols), bf16), dma((4,)), dma],
        input_output_aliases={3: 0},
    )(*parts, early_residual)
    return new_residual.reshape(row_count, width), update


def solution(mesh):
    sections, replicas = mesh.shape["section"], mesh.shape["replica"]
    both = P("section", "replica")
    return jax.shard_map(
        functools.partial(per_device, replicas // NX, NX, sections),
        mesh=mesh,
        in_specs=(both, both, both, both),
        out_specs=(both, both),
        check_vma=False,
    )
```

```python
import functools
import jax
import jax.numpy as jnp
from jax import lax
from jax.experimental import pallas as pl
from jax.experimental.pallas import tpu as pltpu
from jax.sharding import PartitionSpec as P

BLK = 8
LANES = 128
NX = 4
DIRECT = 4
MESH = pl.DeviceIdType.MESH

scale_level = 1.0
epsilon = 1e-06


def ring_far(d, n):
    return min(d, n - d)


def kernel(
    nz, nx, sections,
    grad_hbm, res_hbm, ids_hbm, count_in,
    new_res, summed_out, squares,
    grad, res, packed, packed_ext, rows_out, recv, recv_ext, merged, recv_merged, rows_x, rows_in, square_out, ids_ref,
    column_in, list_sem, load_sem, data_send, data_recv, rows_x_send, rows_x_recv, rows_send, rows_recv, ext_send, ext_recv, merged_send, merged_recv,
    square_send, square_recv,
):
    replicas = nz * nx
    blocks, _, width = grad.shape
    row_count = blocks * BLK
    cols = width // replicas
    slots = ids_ref.shape[1]
    sec, rep = lax.axis_index("section"), lax.axis_index("replica")
    z, x = rep // nx, rep % nx
    others = replicas - 1
    f32, bf16 = jnp.float32, jnp.bfloat16

    column = [((z + d) % nz) * nx + x for d in sorted(range(1, nz), key=lambda d: -ring_far(d, nz))]
    line = {dx: z * nx + (x + dx) % nx for dx in (2, 1, 3)}
    across = [(sec + d) % sections for d in range(1, sections)]
    barrier = pltpu.get_barrier_semaphore()
    for peer in column + list(line.values()):
        pl.semaphore_signal(barrier, inc=1, device_id=(sec, peer), device_id_type=MESH)
    for peer in across:
        pl.semaphore_signal(barrier, inc=1, device_id=(peer, rep), device_id_type=MESH)

    ids_copy = pltpu.make_async_copy(ids_hbm, ids_ref, list_sem)
    ids_copy.start()
    loads = []
    chunks = 4
    step = blocks // chunks
    for c in range(chunks):
        part = pl.ds(c * step, step)
        pair = (
            pltpu.make_async_copy(grad_hbm.at[part], grad.at[part], load_sem.at[0, c]),
            pltpu.make_async_copy(res_hbm.at[part], res.at[part], load_sem.at[1, c]),
        )
        for copy in pair:
            copy.start()
        loads.append(pair)

    ids_copy.wait()
    lane = lax.broadcasted_iota(jnp.int32, (1, LANES), 1)
    group = LANES // (DIRECT * BLK)
    slot_of = lane // BLK - (rep % group) * DIRECT
    count = jnp.broadcast_to(count_in[...], (1, LANES))
    ids = [jnp.full((1, LANES), ids_ref[0, s], jnp.int32) for s in range(slots)]
    ids = [jnp.where(count > s, ids[s], -1) for s in range(slots)]
    base = 2 * row_count
    both_rows = jnp.zeros((1, LANES), jnp.int32)
    for s in range(slots):
        target = jnp.where(ids[s] >= 0, ids[s] * BLK + lane % BLK + 1, 0)
        if s < DIRECT:
            both_rows = both_rows + jnp.where(slot_of == s, target, 0)
        else:
            both_rows = both_rows + jnp.where(slot_of == s - DIRECT, target * base, 0)
    rows_out[0:1] = both_rows
    rows_x[pl.ds(x, 1)] = both_rows

    for c in range(chunks):
        for copy in loads[c]:
            copy.wait()
        for b in range(c * step, (c + 1) * step):
            res[b] = grad[b].astype(f32) + res[b]

    half = nz // 2
    for pair in range(DIRECT // 2, slots // 2):
        picked = []
        for h in range(2):
            s = 2 * pair + h
            alive = jnp.broadcast_to(jnp.where(ids[s] >= 0, 1.0, 0.0), (BLK, LANES))
            alive = jnp.concatenate([alive] * (width // LANES), axis=1)
            picked.append(jnp.where(alive > 0.5, res[ids_ref[0, s]], 0.0))
        both = jnp.concatenate(picked, axis=0).astype(bf16)
        rows = slice((pair - DIRECT // 2) * 2 * BLK, (pair - DIRECT // 2 + 1) * 2 * BLK)
        for zd in range(nz):
            place = (zd // half + z // half + 1) % 2 * half + zd % half
            for xd in range(nx):
                r = zd * nx + xd
                packed_ext[xd, pl.ds(place, 1), rows, :] = both[None, :, r * cols : (r + 1) * cols]
    for pair in range(DIRECT // 2):
        both = jnp.concatenate([res[ids_ref[0, 2 * pair + h]] for h in range(2)], axis=0).astype(bf16)
        rows = slice(pair * 2 * BLK, (pair + 1) * 2 * BLK)
        for r in range(replicas):
            packed[r, rows, :] = both[:, r * cols : (r + 1) * cols]
    recv[pl.ds((half + z % half) * nx + x, 1)] = packed[pl.ds(rep, 1)]
    recv_ext[pl.ds(x, 1)] = packed_ext[pl.ds(x, 1)]

    pl.semaphore_wait(barrier, len(column) + len(line) + len(across))
    for dx in (2, 1, 3):
        pl.semaphore_signal(column_in.at[x], inc=1, device_id=(sec, line[dx]), device_id_type=MESH)

    halves = (pl.ds(0, half), pl.ds(half, half))
    for dx in sorted(range(1, nx), key=lambda d: -ring_far(d, nx)):
        pltpu.make_async_remote_copy(
            rows_out.at[pl.ds(0, 1)], rows_x.at[pl.ds(x, 1)], rows_x_send, rows_x_recv,
            device_id=(sec, z * nx + (x + dx) % nx), device_id_type=MESH,
        ).start()
    def send_ext(h):
        for dx in sorted(range(1, nx), key=lambda d: -ring_far(d, nx)):
            xd = (x + dx) % nx
            pltpu.make_async_remote_copy(
                packed_ext.at[xd, halves[h]], recv_ext.at[x, halves[h]], ext_send.at[h], ext_recv.at[h],
                device_id=(sec, z * nx + xd), device_id_type=MESH,
            ).start()

    def send_to(zt, dx, same):
        to = zt * nx + (x + dx) % nx
        pltpu.make_async_remote_copy(
            packed.at[to], recv.at[(same * half + z % half) * nx + x], data_send, data_recv.at[same],
            device_id=(sec, to), device_id_type=MESH,
        ).start()

    mine_half, other_half = (z // half) * half, (1 - z // half) * half
    cross = [other_half + (z + k) % half for k in (2, 1, 3, 0)]
    inner = [mine_half + (z + k) % half for k in (2, 1, 3)]

    def send_cross(steps):
        for dx in steps:
            for zt in cross:
                send_to(zt, dx, 0)

    def send_inner(steps):
        for dx in steps:
            for zt in inner:
                send_to(zt, dx, 1)
            if dx:
                send_to(z, dx, 1)

    def forward_rows():
        every = rows_x.at[pl.ds(0, nx - 1)]
        pltpu.make_async_copy(every, every, rows_x_recv).wait()
        quad = rows_x[...].sum(axis=0, keepdims=True)
        rows_out[1:2] = quad
        rows_in[pl.ds(half + z % half, 1)] = quad
        for same, places in enumerate((cross, inner)):
            for zt in places:
                pltpu.make_async_remote_copy(
                    rows_out.at[pl.ds(1, 1)], rows_in.at[pl.ds(same * half + z % half, 1)], rows_send, rows_recv,
                    device_id=(sec, zt * nx + x), device_id_type=MESH,
                ).start()

    def forward(h):
        start = h * half
        every = recv_ext.at[pl.ds(0, nx - 1), halves[h]]
        pltpu.make_async_copy(every, every, ext_recv.at[h]).wait()
        total = recv_ext[0, start : start + half]
        for k in range(1, nx):
            total = total + recv_ext[k, start : start + half]
        merged[start : start + half] = total
        for zt in (inner if h else cross):
            pltpu.make_async_remote_copy(
                merged.at[start + zt % half], recv_merged.at[z], merged_send, merged_recv,
                device_id=(sec, zt * nx + x), device_id_type=MESH,
            ).start()
        if h:
            recv_merged[pl.ds(z, 1)] = merged[pl.ds(start + z % half, 1)]

    def column_ready(dx):
        pl.semaphore_wait(column_in.at[(x + dx) % nx], 1)

    send_ext(0)
    send_ext(1)
    send_cross((0,))
    column_ready(1)
    send_cross((1,))
    column_ready(3)
    send_cross((3,))
    column_ready(2)
    send_cross((2,))
    forward_rows()
    forward(0)
    send_inner((2, 1, 3, 0))
    forward(1)

    for b in range(blocks):
        hit = jnp.zeros((1, LANES), f32)
        for s in range(slots):
            hit = jnp.where(ids[s] == b, 1.0, hit)
        kept = jnp.concatenate([jnp.broadcast_to(hit, (BLK, LANES))] * (width // LANES), axis=1)
        mine = res[b]
        new_res[b] = mine - mine.astype(bf16).astype(f32) * kept

    every_row = rows_in.at[pl.ds(0, nz - 1)]
    pltpu.make_async_copy(every_row, every_row, rows_recv).wait()
    row = lax.broadcasted_iota(jnp.int32, (row_count, LANES), 0) + 1
    lists = rows_in[...]
    ext_rows = (lists // base).sum(axis=0, keepdims=True)
    direct_rows = lists % base
    hot_ext = jnp.where(row == ext_rows, 1.0, 0.0).astype(bf16)
    hots = [jnp.where(row == direct_rows[g : g + 1], 1.0, 0.0).astype(bf16) for g in range(replicas // group)]

    summed = jnp.zeros((row_count, cols), f32)
    for same in range(2):
        every = recv.at[pl.ds(same * half * nx, half * nx - same)]
        pltpu.make_async_copy(every, every, data_recv.at[same]).wait()
        for g in range(same * half, (same + 1) * half):
            held = recv[g * group : (g + 1) * group].reshape(LANES, cols)
            summed = summed + jnp.dot(hots[g], held, preferred_element_type=f32)
    every = recv_merged.at[pl.ds(0, nz - 1)]
    pltpu.make_async_copy(every, every, merged_recv).wait()
    ext = recv_merged[0]
    for k in range(1, nz):
        ext = ext + recv_merged[k]
    summed = summed + jnp.dot(hot_ext, jnp.concatenate([ext] * group, axis=0), preferred_element_type=f32)
    summed_out[...] = summed
    device = sec * replicas + rep
    square_out[...] = (summed * summed).reshape(row_count // 8, 8, cols).sum(axis=0).sum(axis=0, keepdims=True)
    squares[pl.ds(device, 1)] = square_out[...]
    def send_square(s_to, r_to):
        pltpu.make_async_remote_copy(
            square_out, squares.at[pl.ds(device, 1)], square_send, square_recv,
            device_id=(s_to, r_to), device_id_type=MESH,
        ).start()
    spread = sorted(
        [(d, dx) for d in range(sections) for dx in range(nx)],
        key=lambda o: (-ring_far(o[0] // 2, sections // 2) - ring_far(o[1], nx), o),
    )
    for zt in (0, 1, 2, 3, 7, 6, 5, 4):
        for d, dx in spread:
            go = functools.partial(send_square, (sec + d) % sections, zt * nx + (x + dx) % nx)
            if (d, dx) == (0, 0):
                pl.when(z != zt)(go)
            else:
                go()
    every_square = squares.at[pl.ds(0, sections * replicas - 1)]
    pltpu.make_async_copy(every_square, every_square, square_recv).wait()
    every = packed.at[pl.ds(0, others)]
    pltpu.make_async_copy(every, every, data_send).wait()
    every = rows_x.at[pl.ds(0, nx - 1)]
    pltpu.make_async_copy(every, every, rows_x_send).wait()
    pltpu.make_async_copy(every_row, every_row, rows_send).wait()
    for h in range(2):
        every = recv_ext.at[pl.ds(0, nx - 1), halves[h]]
        pltpu.make_async_copy(every, every, ext_send.at[h]).wait()
    every = recv_merged.at[pl.ds(0, nz - 1)]
    pltpu.make_async_copy(every, every, merged_send).wait()
    pltpu.make_async_copy(every_square, every_square, square_send).wait()


def released_first(nx):
    sec, rep = lax.axis_index("section"), lax.axis_index("replica")
    y, z, x = sec // 2, rep // nx, rep % nx
    return y + z + jnp.minimum(x, 1) <= 1


def ahead(nx, grad_hbm, res_hbm, ids_hbm, count_ref, new_res_hbm, grad, res, ids_ref, list_sem, load_sem, store_sem):
    @pl.when(released_first(nx))
    def _():
        blocks, _, width = grad.shape
        step = blocks // 4
        parts = [pl.ds(c * step, step) for c in range(4)]
        loads = [
            (
                pltpu.make_async_copy(grad_hbm.at[p], grad.at[p], load_sem.at[0, c]),
                pltpu.make_async_copy(res_hbm.at[p], res.at[p], load_sem.at[1, c]),
            )
            for c, p in enumerate(parts)
        ]
        stores = [pltpu.make_async_copy(res.at[p], new_res_hbm.at[p], store_sem.at[c]) for c, p in enumerate(parts)]
        for pair in loads:
            for copy in pair:
                copy.start()
        ids_copy = pltpu.make_async_copy(ids_hbm, ids_ref, list_sem)
        ids_copy.start()
        ids_copy.wait()
        count = jnp.full((1, LANES), count_ref[0, 0], jnp.int32)
        ids = [jnp.full((1, LANES), ids_ref[0, s], jnp.int32) for s in range(ids_ref.shape[1])]
        for c in range(4):
            for copy in loads[c]:
                copy.wait()
            for b in range(c * step, (c + 1) * step):
                hit = jnp.zeros((1, LANES), jnp.float32)
                for s, one in enumerate(ids):
                    hit = jnp.where((one == b) & (count > s), 1.0, hit)
                kept = jnp.concatenate([jnp.broadcast_to(hit, (BLK, LANES))] * (width // LANES), axis=1)
                mine = grad[b].astype(jnp.float32) + res[b]
                res[b] = mine - mine.astype(jnp.bfloat16).astype(jnp.float32) * kept
            stores[c].start()
        for copy in stores:
            copy.wait()


def finish(count_total, nx, new_res, summed, squares, _, new_res_hbm, update_hbm, update, res_sem, update_sem):
    step = new_res.shape[0] // 4
    copies = [
        pltpu.make_async_copy(new_res.at[pl.ds(c * step, step)], new_res_hbm.at[pl.ds(c * step, step)], res_sem.at[c])
        for c in range(4)
    ]
    late = jnp.logical_not(released_first(nx))

    @pl.when(late)
    def _():
        for copy in copies:
            copy.start()

    every = squares[...]
    norm_total = every.sum(axis=0, keepdims=True).sum(axis=1, keepdims=True)
    clip_factor = scale_level / jnp.sqrt(norm_total / count_total + epsilon)
    update[...] = (summed[...] * clip_factor).astype(jnp.bfloat16)
    last = pltpu.make_async_copy(update, update_hbm, update_sem)
    last.start()

    @pl.when(late)
    def _():
        for copy in copies:
            copy.wait()

    last.wait()


def per_device(nz, nx, sections, gradient, residual, block_ids, block_counts):
    replicas = nz * nx
    row_count, width = gradient.shape
    cols = width // replicas
    slots = block_ids.shape[1]
    count_total = sections * row_count * width
    f32, bf16, i32 = jnp.float32, jnp.bfloat16, jnp.int32
    dma = pltpu.SemaphoreType.DMA
    blocks = row_count // BLK
    shape = (blocks, BLK, width)
    direct_rows, ext_rows = DIRECT * BLK, (slots - DIRECT) * BLK
    gradient, residual = gradient.reshape(shape), residual.reshape(shape)
    in_hbm = pl.BlockSpec(memory_space=pltpu.HBM)
    in_vmem = pl.BlockSpec(memory_space=pltpu.VMEM)
    in_smem = pl.BlockSpec(memory_space=pltpu.SMEM)
    early_residual = pl.pallas_call(
        functools.partial(ahead, nx),
        out_shape=pltpu.HBM(shape, f32),
        in_specs=[in_hbm, in_hbm, in_hbm, in_smem],
        out_specs=in_hbm,
        scratch_shapes=[pltpu.VMEM(shape, bf16), pltpu.VMEM(shape, f32), pltpu.SMEM((1, slots), i32), dma, dma((2, 4)), dma((4,))],
    )(gradient, residual, block_ids, block_counts)
    new_residual, summed, squares = pl.pallas_call(
        functools.partial(kernel, nz, nx, sections),
        out_shape=(
            pltpu.VMEM(shape, f32), pltpu.VMEM((row_count, cols), f32), pltpu.VMEM((sections * replicas, cols), f32)
        ),
        in_specs=[pl.BlockSpec(memory_space=pltpu.HBM)] * 3 + [pl.BlockSpec(memory_space=pltpu.VMEM)],
        out_specs=(pl.BlockSpec(memory_space=pltpu.VMEM),) * 3,
        scratch_shapes=[
            pltpu.VMEM(shape, bf16),
            pltpu.VMEM(shape, f32),
            pltpu.VMEM((replicas, direct_rows, cols), bf16),
            pltpu.VMEM((nx, nz, ext_rows, cols), bf16),
            pltpu.VMEM((2, LANES), i32),
            pltpu.VMEM((replicas, direct_rows, cols), bf16),
            pltpu.VMEM((nx, nz, ext_rows, cols), bf16),
            pltpu.VMEM((nz, ext_rows, cols), bf16),
            pltpu.VMEM((nz, ext_rows, cols), bf16),
            pltpu.VMEM((nx, LANES), i32),
            pltpu.VMEM((nz, LANES), i32),
            pltpu.VMEM((1, cols), f32),
            pltpu.SMEM((1, slots), i32),
            pltpu.SemaphoreType.REGULAR((nx,)), dma, dma((2, 4)), dma, dma((2,)), dma, dma, dma, dma, dma((2,)), dma((2,)), dma, dma, dma, dma,
        ],
        compiler_params=pltpu.CompilerParams(collective_id=0, has_side_effects=True),
    )(gradient, residual, block_ids, block_counts)
    parts = (pltpu.with_memory_space_constraint(v, pltpu.VMEM) for v in (new_residual, summed, squares))
    new_residual, update = pl.pallas_call(
        functools.partial(finish, count_total, nx),
        out_shape=(pltpu.HBM(shape, f32), pltpu.HBM((row_count, cols), bf16)),
        in_specs=[in_vmem] * 3 + [in_hbm],
        out_specs=(in_hbm, in_hbm),
        scratch_shapes=[pltpu.VMEM((row_count, cols), bf16), dma((4,)), dma],
        input_output_aliases={3: 0},
    )(*parts, early_residual)
    return new_residual.reshape(row_count, width), update


def solution(mesh):
    sections, replicas = mesh.shape["section"], mesh.shape["replica"]
    both = P("section", "replica")
    return jax.shard_map(
        functools.partial(per_device, replicas // NX, NX, sections),
        mesh=mesh,
        in_specs=(both, both, both, both),
        out_specs=(both, both),
        check_vma=False,
    )
```

```python
import functools
import jax
import jax.numpy as jnp
from jax import lax
from jax.experimental import pallas as pl
from jax.experimental.pallas import tpu as pltpu
from jax.sharding import PartitionSpec as P

BLK = 8
LANES = 128
NX = 4
DIRECT = 4
MESH = pl.DeviceIdType.MESH

scale_level = 1.0
epsilon = 1e-06


def ring_far(d, n):
    return min(d, n - d)


def kernel(
    nz, nx, sections,
    grad_hbm, res_hbm, ids_hbm, count_in,
    new_res, summed_out, squares,
    grad, res, packed, packed_ext, rows_out, recv, recv_ext, merged, recv_merged, rows_x, rows_in, square_out, ids_ref,
    column_in, list_sem, load_sem, data_send, data_recv, rows_x_send, rows_x_recv, rows_send, rows_recv, ext_send, ext_recv, merged_send, merged_recv,
    square_send, square_recv,
):
    replicas = nz * nx
    blocks, _, width = grad.shape
    row_count = blocks * BLK
    cols = width // replicas
    slots = ids_ref.shape[1]
    sec, rep = lax.axis_index("section"), lax.axis_index("replica")
    z, x = rep // nx, rep % nx
    others = replicas - 1
    f32, bf16 = jnp.float32, jnp.bfloat16

    column = [((z + d) % nz) * nx + x for d in sorted(range(1, nz), key=lambda d: -ring_far(d, nz))]
    line = {dx: z * nx + (x + dx) % nx for dx in (2, 1, 3)}
    across = [(sec + d) % sections for d in range(1, sections)]
    barrier = pltpu.get_barrier_semaphore()
    for peer in column + list(line.values()):
        pl.semaphore_signal(barrier, inc=1, device_id=(sec, peer), device_id_type=MESH)
    for peer in across:
        pl.semaphore_signal(barrier, inc=1, device_id=(peer, rep), device_id_type=MESH)

    ids_copy = pltpu.make_async_copy(ids_hbm, ids_ref, list_sem)
    ids_copy.start()
    loads = []
    chunks = 4
    step = blocks // chunks
    for c in range(chunks):
        part = pl.ds(c * step, step)
        pair = (
            pltpu.make_async_copy(grad_hbm.at[part], grad.at[part], load_sem.at[0, c]),
            pltpu.make_async_copy(res_hbm.at[part], res.at[part], load_sem.at[1, c]),
        )
        for copy in pair:
            copy.start()
        loads.append(pair)

    ids_copy.wait()
    lane = lax.broadcasted_iota(jnp.int32, (1, LANES), 1)
    group = LANES // (DIRECT * BLK)
    slot_of = lane // BLK - (rep % group) * DIRECT
    count = jnp.broadcast_to(count_in[...], (1, LANES))
    ids = [jnp.full((1, LANES), ids_ref[0, s], jnp.int32) for s in range(slots)]
    ids = [jnp.where(count > s, ids[s], -1) for s in range(slots)]
    base = 2 * row_count
    both_rows = jnp.zeros((1, LANES), jnp.int32)
    for s in range(slots):
        target = jnp.where(ids[s] >= 0, ids[s] * BLK + lane % BLK + 1, 0)
        if s < DIRECT:
            both_rows = both_rows + jnp.where(slot_of == s, target, 0)
        else:
            both_rows = both_rows + jnp.where(slot_of == s - DIRECT, target * base, 0)
    rows_out[0:1] = both_rows
    rows_x[pl.ds(x, 1)] = both_rows

    for c in range(chunks):
        for copy in loads[c]:
            copy.wait()
        for b in range(c * step, (c + 1) * step):
            res[b] = grad[b].astype(f32) + res[b]

    half = nz // 2
    for pair in range(DIRECT // 2, slots // 2):
        picked = []
        for h in range(2):
            s = 2 * pair + h
            alive = jnp.broadcast_to(jnp.where(ids[s] >= 0, 1.0, 0.0), (BLK, LANES))
            alive = jnp.concatenate([alive] * (width // LANES), axis=1)
            picked.append(jnp.where(alive > 0.5, res[ids_ref[0, s]], 0.0))
        both = jnp.concatenate(picked, axis=0).astype(bf16)
        rows = slice((pair - DIRECT // 2) * 2 * BLK, (pair - DIRECT // 2 + 1) * 2 * BLK)
        for zd in range(nz):
            place = (zd // half + z // half + 1) % 2 * half + zd % half
            for xd in range(nx):
                r = zd * nx + xd
                packed_ext[xd, pl.ds(place, 1), rows, :] = both[None, :, r * cols : (r + 1) * cols]
    for pair in range(DIRECT // 2):
        both = jnp.concatenate([res[ids_ref[0, 2 * pair + h]] for h in range(2)], axis=0).astype(bf16)
        rows = slice(pair * 2 * BLK, (pair + 1) * 2 * BLK)
        for r in range(replicas):
            packed[r, rows, :] = both[:, r * cols : (r + 1) * cols]
    recv[pl.ds((half + z % half) * nx + x, 1)] = packed[pl.ds(rep, 1)]
    recv_ext[pl.ds(x, 1)] = packed_ext[pl.ds(x, 1)]

    pl.semaphore_wait(barrier, len(column) + len(line) + len(across))
    for dx in (2, 1, 3):
        pl.semaphore_signal(column_in.at[x], inc=1, device_id=(sec, line[dx]), device_id_type=MESH)

    halves = (pl.ds(0, half), pl.ds(half, half))
    for dx in sorted(range(1, nx), key=lambda d: -ring_far(d, nx)):
        pltpu.make_async_remote_copy(
            rows_out.at[pl.ds(0, 1)], rows_x.at[pl.ds(x, 1)], rows_x_send, rows_x_recv,
            device_id=(sec, z * nx + (x + dx) % nx), device_id_type=MESH,
        ).start()
    def send_ext(h):
        for dx in sorted(range(1, nx), key=lambda d: -ring_far(d, nx)):
            xd = (x + dx) % nx
            pltpu.make_async_remote_copy(
                packed_ext.at[xd, halves[h]], recv_ext.at[x, halves[h]], ext_send.at[h], ext_recv.at[h],
                device_id=(sec, z * nx + xd), device_id_type=MESH,
            ).start()

    def send_to(zt, dx, same):
        to = zt * nx + (x + dx) % nx
        pltpu.make_async_remote_copy(
            packed.at[to], recv.at[(same * half + z % half) * nx + x], data_send, data_recv.at[same],
            device_id=(sec, to), device_id_type=MESH,
        ).start()

    mine_half, other_half = (z // half) * half, (1 - z // half) * half
    cross = [other_half + (z + k) % half for k in (2, 1, 3, 0)]
    inner = [mine_half + (z + k) % half for k in (2, 1, 3)]

    def send_cross(steps):
        for dx in steps:
            for zt in cross:
                send_to(zt, dx, 0)

    def send_inner(steps):
        for dx in steps:
            for zt in inner:
                send_to(zt, dx, 1)
            if dx:
                send_to(z, dx, 1)

    def forward_rows():
        every = rows_x.at[pl.ds(0, nx - 1)]
        pltpu.make_async_copy(every, every, rows_x_recv).wait()
        quad = rows_x[...].sum(axis=0, keepdims=True)
        rows_out[1:2] = quad
        rows_in[pl.ds(half + z % half, 1)] = quad
        for same, places in enumerate((cross, inner)):
            for zt in places:
                pltpu.make_async_remote_copy(
                    rows_out.at[pl.ds(1, 1)], rows_in.at[pl.ds(same * half + z % half, 1)], rows_send, rows_recv,
                    device_id=(sec, zt * nx + x), device_id_type=MESH,
                ).start()

    def forward(h):
        start = h * half
        every = recv_ext.at[pl.ds(0, nx - 1), halves[h]]
        pltpu.make_async_copy(every, every, ext_recv.at[h]).wait()
        total = recv_ext[0, start : start + half]
        for k in range(1, nx):
            total = total + recv_ext[k, start : start + half]
        merged[start : start + half] = total
        for zt in (inner if h else cross):
            pltpu.make_async_remote_copy(
                merged.at[start + zt % half], recv_merged.at[z], merged_send, merged_recv,
                device_id=(sec, zt * nx + x), device_id_type=MESH,
            ).start()
        if h:
            recv_merged[pl.ds(z, 1)] = merged[pl.ds(start + z % half, 1)]

    def column_ready(dx):
        pl.semaphore_wait(column_in.at[(x + dx) % nx], 1)

    send_ext(0)
    send_ext(1)
    send_cross((0,))
    column_ready(1)
    send_cross((1,))
    column_ready(3)
    send_cross((3,))
    column_ready(2)
    send_cross((2,))
    send_inner((0, 2))
    forward_rows()
    forward(0)
    send_inner((1, 3))
    forward(1)

    for b in range(blocks):
        hit = jnp.zeros((1, LANES), f32)
        for s in range(slots):
            hit = jnp.where(ids[s] == b, 1.0, hit)
        kept = jnp.concatenate([jnp.broadcast_to(hit, (BLK, LANES))] * (width // LANES), axis=1)
        mine = res[b]
        new_res[b] = mine - mine.astype(bf16).astype(f32) * kept

    every_row = rows_in.at[pl.ds(0, nz - 1)]
    pltpu.make_async_copy(every_row, every_row, rows_recv).wait()
    row = lax.broadcasted_iota(jnp.int32, (row_count, LANES), 0) + 1
    lists = rows_in[...]
    ext_rows = (lists // base).sum(axis=0, keepdims=True)
    direct_rows = lists % base
    hot_ext = jnp.where(row == ext_rows, 1.0, 0.0).astype(bf16)
    hots = [jnp.where(row == direct_rows[g : g + 1], 1.0, 0.0).astype(bf16) for g in range(replicas // group)]

    summed = jnp.zeros((row_count, cols), f32)
    for same in range(2):
        every = recv.at[pl.ds(same * half * nx, half * nx - same)]
        pltpu.make_async_copy(every, every, data_recv.at[same]).wait()
        for g in range(same * half, (same + 1) * half):
            held = recv[g * group : (g + 1) * group].reshape(LANES, cols)
            summed = summed + jnp.dot(hots[g], held, preferred_element_type=f32)
    every = recv_merged.at[pl.ds(0, nz - 1)]
    pltpu.make_async_copy(every, every, merged_recv).wait()
    ext = recv_merged[0]
    for k in range(1, nz):
        ext = ext + recv_merged[k]
    summed = summed + jnp.dot(hot_ext, jnp.concatenate([ext] * group, axis=0), preferred_element_type=f32)
    summed_out[...] = summed
    device = sec * replicas + rep
    square_out[...] = (summed * summed).reshape(row_count // 8, 8, cols).sum(axis=0).sum(axis=0, keepdims=True)
    squares[pl.ds(device, 1)] = square_out[...]
    def send_square(s_to, r_to):
        pltpu.make_async_remote_copy(
            square_out, squares.at[pl.ds(device, 1)], square_send, square_recv,
            device_id=(s_to, r_to), device_id_type=MESH,
        ).start()
    spread = sorted(
        [(d, dx) for d in range(sections) for dx in range(nx)],
        key=lambda o: (-ring_far(o[0] // 2, sections // 2) - ring_far(o[1], nx), o),
    )
    for zt in (0, 1, 2, 3, 7, 6, 5, 4):
        for d, dx in spread:
            go = functools.partial(send_square, (sec + d) % sections, zt * nx + (x + dx) % nx)
            if (d, dx) == (0, 0):
                pl.when(z != zt)(go)
            else:
                go()
    every_square = squares.at[pl.ds(0, sections * replicas - 1)]
    pltpu.make_async_copy(every_square, every_square, square_recv).wait()
    every = packed.at[pl.ds(0, others)]
    pltpu.make_async_copy(every, every, data_send).wait()
    every = rows_x.at[pl.ds(0, nx - 1)]
    pltpu.make_async_copy(every, every, rows_x_send).wait()
    pltpu.make_async_copy(every_row, every_row, rows_send).wait()
    for h in range(2):
        every = recv_ext.at[pl.ds(0, nx - 1), halves[h]]
        pltpu.make_async_copy(every, every, ext_send.at[h]).wait()
    every = recv_merged.at[pl.ds(0, nz - 1)]
    pltpu.make_async_copy(every, every, merged_send).wait()
    pltpu.make_async_copy(every_square, every_square, square_send).wait()


def released_first(nx):
    sec, rep = lax.axis_index("section"), lax.axis_index("replica")
    y, z, x = sec // 2, rep // nx, rep % nx
    return y + z + jnp.minimum(x, 1) <= 1


def ahead(nx, grad_hbm, res_hbm, ids_hbm, count_ref, new_res_hbm, grad, res, ids_ref, list_sem, load_sem, store_sem):
    @pl.when(released_first(nx))
    def _():
        blocks, _, width = grad.shape
        step = blocks // 4
        parts = [pl.ds(c * step, step) for c in range(4)]
        loads = [
            (
                pltpu.make_async_copy(grad_hbm.at[p], grad.at[p], load_sem.at[0, c]),
                pltpu.make_async_copy(res_hbm.at[p], res.at[p], load_sem.at[1, c]),
            )
            for c, p in enumerate(parts)
        ]
        stores = [pltpu.make_async_copy(res.at[p], new_res_hbm.at[p], store_sem.at[c]) for c, p in enumerate(parts)]
        for pair in loads:
            for copy in pair:
                copy.start()
        ids_copy = pltpu.make_async_copy(ids_hbm, ids_ref, list_sem)
        ids_copy.start()
        ids_copy.wait()
        count = jnp.full((1, LANES), count_ref[0, 0], jnp.int32)
        ids = [jnp.full((1, LANES), ids_ref[0, s], jnp.int32) for s in range(ids_ref.shape[1])]
        for c in range(4):
            for copy in loads[c]:
                copy.wait()
            for b in range(c * step, (c + 1) * step):
                hit = jnp.zeros((1, LANES), jnp.float32)
                for s, one in enumerate(ids):
                    hit = jnp.where((one == b) & (count > s), 1.0, hit)
                kept = jnp.concatenate([jnp.broadcast_to(hit, (BLK, LANES))] * (width // LANES), axis=1)
                mine = grad[b].astype(jnp.float32) + res[b]
                res[b] = mine - mine.astype(jnp.bfloat16).astype(jnp.float32) * kept
            stores[c].start()
        for copy in stores:
            copy.wait()


def finish(count_total, nx, new_res, summed, squares, _, new_res_hbm, update_hbm, update, res_sem, update_sem):
    step = new_res.shape[0] // 4
    copies = [
        pltpu.make_async_copy(new_res.at[pl.ds(c * step, step)], new_res_hbm.at[pl.ds(c * step, step)], res_sem.at[c])
        for c in range(4)
    ]
    late = jnp.logical_not(released_first(nx))

    @pl.when(late)
    def _():
        for copy in copies:
            copy.start()

    every = squares[...]
    norm_total = every.sum(axis=0, keepdims=True).sum(axis=1, keepdims=True)
    clip_factor = scale_level / jnp.sqrt(norm_total / count_total + epsilon)
    update[...] = (summed[...] * clip_factor).astype(jnp.bfloat16)
    last = pltpu.make_async_copy(update, update_hbm, update_sem)
    last.start()

    @pl.when(late)
    def _():
        for copy in copies:
            copy.wait()

    last.wait()


def per_device(nz, nx, sections, gradient, residual, block_ids, block_counts):
    replicas = nz * nx
    row_count, width = gradient.shape
    cols = width // replicas
    slots = block_ids.shape[1]
    count_total = sections * row_count * width
    f32, bf16, i32 = jnp.float32, jnp.bfloat16, jnp.int32
    dma = pltpu.SemaphoreType.DMA
    blocks = row_count // BLK
    shape = (blocks, BLK, width)
    direct_rows, ext_rows = DIRECT * BLK, (slots - DIRECT) * BLK
    gradient, residual = gradient.reshape(shape), residual.reshape(shape)
    in_hbm = pl.BlockSpec(memory_space=pltpu.HBM)
    in_vmem = pl.BlockSpec(memory_space=pltpu.VMEM)
    in_smem = pl.BlockSpec(memory_space=pltpu.SMEM)
    early_residual = pl.pallas_call(
        functools.partial(ahead, nx),
        out_shape=pltpu.HBM(shape, f32),
        in_specs=[in_hbm, in_hbm, in_hbm, in_smem],
        out_specs=in_hbm,
        scratch_shapes=[pltpu.VMEM(shape, bf16), pltpu.VMEM(shape, f32), pltpu.SMEM((1, slots), i32), dma, dma((2, 4)), dma((4,))],
    )(gradient, residual, block_ids, block_counts)
    new_residual, summed, squares = pl.pallas_call(
        functools.partial(kernel, nz, nx, sections),
        out_shape=(
            pltpu.VMEM(shape, f32), pltpu.VMEM((row_count, cols), f32), pltpu.VMEM((sections * replicas, cols), f32)
        ),
        in_specs=[pl.BlockSpec(memory_space=pltpu.HBM)] * 3 + [pl.BlockSpec(memory_space=pltpu.VMEM)],
        out_specs=(pl.BlockSpec(memory_space=pltpu.VMEM),) * 3,
        scratch_shapes=[
            pltpu.VMEM(shape, bf16),
            pltpu.VMEM(shape, f32),
            pltpu.VMEM((replicas, direct_rows, cols), bf16),
            pltpu.VMEM((nx, nz, ext_rows, cols), bf16),
            pltpu.VMEM((2, LANES), i32),
            pltpu.VMEM((replicas, direct_rows, cols), bf16),
            pltpu.VMEM((nx, nz, ext_rows, cols), bf16),
            pltpu.VMEM((nz, ext_rows, cols), bf16),
            pltpu.VMEM((nz, ext_rows, cols), bf16),
            pltpu.VMEM((nx, LANES), i32),
            pltpu.VMEM((nz, LANES), i32),
            pltpu.VMEM((1, cols), f32),
            pltpu.SMEM((1, slots), i32),
            pltpu.SemaphoreType.REGULAR((nx,)), dma, dma((2, 4)), dma, dma((2,)), dma, dma, dma, dma, dma((2,)), dma((2,)), dma, dma, dma, dma,
        ],
        compiler_params=pltpu.CompilerParams(collective_id=0, has_side_effects=True),
    )(gradient, residual, block_ids, block_counts)
    parts = (pltpu.with_memory_space_constraint(v, pltpu.VMEM) for v in (new_residual, summed, squares))
    new_residual, update = pl.pallas_call(
        functools.partial(finish, count_total, nx),
        out_shape=(pltpu.HBM(shape, f32), pltpu.HBM((row_count, cols), bf16)),
        in_specs=[in_vmem] * 3 + [in_hbm],
        out_specs=(in_hbm, in_hbm),
        scratch_shapes=[pltpu.VMEM((row_count, cols), bf16), dma((4,)), dma],
        input_output_aliases={3: 0},
    )(*parts, early_residual)
    return new_residual.reshape(row_count, width), update


def solution(mesh):
    sections, replicas = mesh.shape["section"], mesh.shape["replica"]
    both = P("section", "replica")
    return jax.shard_map(
        functools.partial(per_device, replicas // NX, NX, sections),
        mesh=mesh,
        in_specs=(both, both, both, both),
        out_specs=(both, both),
        check_vma=False,
    )
```

```python
import functools
import jax
import jax.numpy as jnp
from jax import lax
from jax.experimental import pallas as pl
from jax.experimental.pallas import tpu as pltpu
from jax.sharding import PartitionSpec as P

BLK = 8
LANES = 128
NX = 4
DIRECT = 4
MESH = pl.DeviceIdType.MESH

scale_level = 1.0
epsilon = 1e-06


def ring_far(d, n):
    return min(d, n - d)


def kernel(
    nz, nx, sections,
    grad_hbm, res_hbm, ids_hbm, count_in,
    new_res, summed_out, squares,
    grad, res, packed, packed_ext, rows_out, recv, recv_ext, merged, recv_merged, rows_x, rows_in, square_out, ids_ref,
    column_in, list_sem, load_sem, data_send, data_recv, rows_x_send, rows_x_recv, rows_send, rows_recv, ext_send, ext_recv, merged_send, merged_recv,
    square_send, square_recv,
):
    replicas = nz * nx
    blocks, _, width = grad.shape
    row_count = blocks * BLK
    cols = width // replicas
    slots = ids_ref.shape[1]
    sec, rep = lax.axis_index("section"), lax.axis_index("replica")
    z, x = rep // nx, rep % nx
    others = replicas - 1
    f32, bf16 = jnp.float32, jnp.bfloat16

    column = [((z + d) % nz) * nx + x for d in sorted(range(1, nz), key=lambda d: -ring_far(d, nz))]
    line = {dx: z * nx + (x + dx) % nx for dx in (2, 1, 3)}
    across = [(sec + d) % sections for d in range(1, sections)]
    barrier = pltpu.get_barrier_semaphore()
    for peer in column + list(line.values()):
        pl.semaphore_signal(barrier, inc=1, device_id=(sec, peer), device_id_type=MESH)
    for peer in across:
        pl.semaphore_signal(barrier, inc=1, device_id=(peer, rep), device_id_type=MESH)

    ids_copy = pltpu.make_async_copy(ids_hbm, ids_ref, list_sem)
    ids_copy.start()
    loads = []
    chunks = 4
    step = blocks // chunks
    for c in range(chunks):
        part = pl.ds(c * step, step)
        pair = (
            pltpu.make_async_copy(grad_hbm.at[part], grad.at[part], load_sem.at[0, c]),
            pltpu.make_async_copy(res_hbm.at[part], res.at[part], load_sem.at[1, c]),
        )
        for copy in pair:
            copy.start()
        loads.append(pair)

    ids_copy.wait()
    lane = lax.broadcasted_iota(jnp.int32, (1, LANES), 1)
    group = LANES // (DIRECT * BLK)
    slot_of = lane // BLK - (rep % group) * DIRECT
    count = jnp.broadcast_to(count_in[...], (1, LANES))
    ids = [jnp.full((1, LANES), ids_ref[0, s], jnp.int32) for s in range(slots)]
    ids = [jnp.where(count > s, ids[s], -1) for s in range(slots)]
    base = 2 * row_count
    both_rows = jnp.zeros((1, LANES), jnp.int32)
    for s in range(slots):
        target = jnp.where(ids[s] >= 0, ids[s] * BLK + lane % BLK + 1, 0)
        if s < DIRECT:
            both_rows = both_rows + jnp.where(slot_of == s, target, 0)
        else:
            both_rows = both_rows + jnp.where(slot_of == s - DIRECT, target * base, 0)
    rows_out[0:1] = both_rows
    rows_x[pl.ds(x, 1)] = both_rows

    for c in range(chunks):
        for copy in loads[c]:
            copy.wait()
        for b in range(c * step, (c + 1) * step):
            res[b] = grad[b].astype(f32) + res[b]

    half = nz // 2
    for pair in range(DIRECT // 2, slots // 2):
        picked = []
        for h in range(2):
            s = 2 * pair + h
            alive = jnp.broadcast_to(jnp.where(ids[s] >= 0, 1.0, 0.0), (BLK, LANES))
            alive = jnp.concatenate([alive] * (width // LANES), axis=1)
            picked.append(jnp.where(alive > 0.5, res[ids_ref[0, s]], 0.0))
        both = jnp.concatenate(picked, axis=0).astype(bf16)
        rows = slice((pair - DIRECT // 2) * 2 * BLK, (pair - DIRECT // 2 + 1) * 2 * BLK)
        for zd in range(nz):
            place = (zd // half + z // half + 1) % 2 * half + zd % half
            for xd in range(nx):
                r = zd * nx + xd
                packed_ext[xd, pl.ds(place, 1), rows, :] = both[None, :, r * cols : (r + 1) * cols]
    for pair in range(DIRECT // 2):
        both = jnp.concatenate([res[ids_ref[0, 2 * pair + h]] for h in range(2)], axis=0).astype(bf16)
        rows = slice(pair * 2 * BLK, (pair + 1) * 2 * BLK)
        for r in range(replicas):
            packed[r, rows, :] = both[:, r * cols : (r + 1) * cols]
    recv[pl.ds((half + z % half) * nx + x, 1)] = packed[pl.ds(rep, 1)]
    recv_ext[pl.ds(x, 1)] = packed_ext[pl.ds(x, 1)]

    pl.semaphore_wait(barrier, len(column) + len(line) + len(across))
    for dx in (2, 1, 3):
        pl.semaphore_signal(column_in.at[x], inc=1, device_id=(sec, line[dx]), device_id_type=MESH)

    halves = (pl.ds(0, half), pl.ds(half, half))
    for dx in sorted(range(1, nx), key=lambda d: -ring_far(d, nx)):
        pltpu.make_async_remote_copy(
            rows_out.at[pl.ds(0, 1)], rows_x.at[pl.ds(x, 1)], rows_x_send, rows_x_recv,
            device_id=(sec, z * nx + (x + dx) % nx), device_id_type=MESH,
        ).start()
    def send_ext(h):
        for dx in sorted(range(1, nx), key=lambda d: -ring_far(d, nx)):
            xd = (x + dx) % nx
            pltpu.make_async_remote_copy(
                packed_ext.at[xd, halves[h]], recv_ext.at[x, halves[h]], ext_send.at[h], ext_recv.at[h],
                device_id=(sec, z * nx + xd), device_id_type=MESH,
            ).start()

    def send_to(zt, dx, same):
        to = zt * nx + (x + dx) % nx
        pltpu.make_async_remote_copy(
            packed.at[to], recv.at[(same * half + z % half) * nx + x], data_send, data_recv.at[same],
            device_id=(sec, to), device_id_type=MESH,
        ).start()

    mine_half, other_half = (z // half) * half, (1 - z // half) * half
    cross = [other_half + (z + k) % half for k in (2, 1, 3, 0)]
    inner = [mine_half + (z + k) % half for k in (2, 1, 3)]

    def send_cross(steps):
        for dx in steps:
            for zt in cross:
                send_to(zt, dx, 0)

    def send_inner(steps):
        for dx in steps:
            for zt in inner:
                send_to(zt, dx, 1)
            if dx:
                send_to(z, dx, 1)

    def forward_rows():
        every = rows_x.at[pl.ds(0, nx - 1)]
        pltpu.make_async_copy(every, every, rows_x_recv).wait()
        quad = rows_x[...].sum(axis=0, keepdims=True)
        rows_out[1:2] = quad
        rows_in[pl.ds(half + z % half, 1)] = quad
        for same, places in enumerate((cross, inner)):
            for zt in places:
                pltpu.make_async_remote_copy(
                    rows_out.at[pl.ds(1, 1)], rows_in.at[pl.ds(same * half + z % half, 1)], rows_send, rows_recv,
                    device_id=(sec, zt * nx + x), device_id_type=MESH,
                ).start()

    def forward(h):
        start = h * half
        every = recv_ext.at[pl.ds(0, nx - 1), halves[h]]
        pltpu.make_async_copy(every, every, ext_recv.at[h]).wait()
        total = recv_ext[0, start : start + half]
        for k in range(1, nx):
            total = total + recv_ext[k, start : start + half]
        merged[start : start + half] = total
        for zt in (inner if h else cross):
            pltpu.make_async_remote_copy(
                merged.at[start + zt % half], recv_merged.at[z], merged_send, merged_recv,
                device_id=(sec, zt * nx + x), device_id_type=MESH,
            ).start()
        if h:
            recv_merged[pl.ds(z, 1)] = merged[pl.ds(start + z % half, 1)]

    def column_ready(dx):
        pl.semaphore_wait(column_in.at[(x + dx) % nx], 1)

    send_ext(0)
    send_ext(1)
    send_cross((0,))
    send_inner((0,))
    column_ready(1)
    send_cross((1,))
    column_ready(3)
    send_cross((3,))
    column_ready(2)
    send_cross((2,))
    send_inner((2,))
    forward_rows()
    forward(0)
    send_inner((1, 3))
    forward(1)

    for b in range(blocks):
        hit = jnp.zeros((1, LANES), f32)
        for s in range(slots):
            hit = jnp.where(ids[s] == b, 1.0, hit)
        kept = jnp.concatenate([jnp.broadcast_to(hit, (BLK, LANES))] * (width // LANES), axis=1)
        mine = res[b]
        new_res[b] = mine - mine.astype(bf16).astype(f32) * kept

    every_row = rows_in.at[pl.ds(0, nz - 1)]
    pltpu.make_async_copy(every_row, every_row, rows_recv).wait()
    row = lax.broadcasted_iota(jnp.int32, (row_count, LANES), 0) + 1
    lists = rows_in[...]
    ext_rows = (lists // base).sum(axis=0, keepdims=True)
    direct_rows = lists % base
    hot_ext = jnp.where(row == ext_rows, 1.0, 0.0).astype(bf16)
    hots = [jnp.where(row == direct_rows[g : g + 1], 1.0, 0.0).astype(bf16) for g in range(replicas // group)]

    summed = jnp.zeros((row_count, cols), f32)
    for same in range(2):
        every = recv.at[pl.ds(same * half * nx, half * nx - same)]
        pltpu.make_async_copy(every, every, data_recv.at[same]).wait()
        for g in range(same * half, (same + 1) * half):
            held = recv[g * group : (g + 1) * group].reshape(LANES, cols)
            summed = summed + jnp.dot(hots[g], held, preferred_element_type=f32)
    every = recv_merged.at[pl.ds(0, nz - 1)]
    pltpu.make_async_copy(every, every, merged_recv).wait()
    ext = recv_merged[0]
    for k in range(1, nz):
        ext = ext + recv_merged[k]
    summed = summed + jnp.dot(hot_ext, jnp.concatenate([ext] * group, axis=0), preferred_element_type=f32)
    summed_out[...] = summed
    device = sec * replicas + rep
    square_out[...] = (summed * summed).reshape(row_count // 8, 8, cols).sum(axis=0).sum(axis=0, keepdims=True)
    squares[pl.ds(device, 1)] = square_out[...]
    def send_square(s_to, r_to):
        pltpu.make_async_remote_copy(
            square_out, squares.at[pl.ds(device, 1)], square_send, square_recv,
            device_id=(s_to, r_to), device_id_type=MESH,
        ).start()
    spread = sorted(
        [(d, dx) for d in range(sections) for dx in range(nx)],
        key=lambda o: (-ring_far(o[0] // 2, sections // 2) - ring_far(o[1], nx), o),
    )
    for zt in (0, 1, 2, 3, 7, 6, 5, 4):
        for d, dx in spread:
            go = functools.partial(send_square, (sec + d) % sections, zt * nx + (x + dx) % nx)
            if (d, dx) == (0, 0):
                pl.when(z != zt)(go)
            else:
                go()
    every_square = squares.at[pl.ds(0, sections * replicas - 1)]
    pltpu.make_async_copy(every_square, every_square, square_recv).wait()
    every = packed.at[pl.ds(0, others)]
    pltpu.make_async_copy(every, every, data_send).wait()
    every = rows_x.at[pl.ds(0, nx - 1)]
    pltpu.make_async_copy(every, every, rows_x_send).wait()
    pltpu.make_async_copy(every_row, every_row, rows_send).wait()
    for h in range(2):
        every = recv_ext.at[pl.ds(0, nx - 1), halves[h]]
        pltpu.make_async_copy(every, every, ext_send.at[h]).wait()
    every = recv_merged.at[pl.ds(0, nz - 1)]
    pltpu.make_async_copy(every, every, merged_send).wait()
    pltpu.make_async_copy(every_square, every_square, square_send).wait()


def released_first(nx):
    sec, rep = lax.axis_index("section"), lax.axis_index("replica")
    y, z, x = sec // 2, rep // nx, rep % nx
    return y + z + jnp.minimum(x, 1) <= 1


def ahead(nx, grad_hbm, res_hbm, ids_hbm, count_ref, new_res_hbm, grad, res, ids_ref, list_sem, load_sem, store_sem):
    @pl.when(released_first(nx))
    def _():
        blocks, _, width = grad.shape
        step = blocks // 4
        parts = [pl.ds(c * step, step) for c in range(4)]
        loads = [
            (
                pltpu.make_async_copy(grad_hbm.at[p], grad.at[p], load_sem.at[0, c]),
                pltpu.make_async_copy(res_hbm.at[p], res.at[p], load_sem.at[1, c]),
            )
            for c, p in enumerate(parts)
        ]
        stores = [pltpu.make_async_copy(res.at[p], new_res_hbm.at[p], store_sem.at[c]) for c, p in enumerate(parts)]
        for pair in loads:
            for copy in pair:
                copy.start()
        ids_copy = pltpu.make_async_copy(ids_hbm, ids_ref, list_sem)
        ids_copy.start()
        ids_copy.wait()
        count = jnp.full((1, LANES), count_ref[0, 0], jnp.int32)
        ids = [jnp.full((1, LANES), ids_ref[0, s], jnp.int32) for s in range(ids_ref.shape[1])]
        for c in range(4):
            for copy in loads[c]:
                copy.wait()
            for b in range(c * step, (c + 1) * step):
                hit = jnp.zeros((1, LANES), jnp.float32)
                for s, one in enumerate(ids):
                    hit = jnp.where((one == b) & (count > s), 1.0, hit)
                kept = jnp.concatenate([jnp.broadcast_to(hit, (BLK, LANES))] * (width // LANES), axis=1)
                mine = grad[b].astype(jnp.float32) + res[b]
                res[b] = mine - mine.astype(jnp.bfloat16).astype(jnp.float32) * kept
            stores[c].start()
        for copy in stores:
            copy.wait()


def finish(count_total, nx, new_res, summed, squares, _, new_res_hbm, update_hbm, update, res_sem, update_sem):
    step = new_res.shape[0] // 4
    copies = [
        pltpu.make_async_copy(new_res.at[pl.ds(c * step, step)], new_res_hbm.at[pl.ds(c * step, step)], res_sem.at[c])
        for c in range(4)
    ]
    late = jnp.logical_not(released_first(nx))

    @pl.when(late)
    def _():
        for copy in copies:
            copy.start()

    every = squares[...]
    norm_total = every.sum(axis=0, keepdims=True).sum(axis=1, keepdims=True)
    clip_factor = scale_level / jnp.sqrt(norm_total / count_total + epsilon)
    update[...] = (summed[...] * clip_factor).astype(jnp.bfloat16)
    last = pltpu.make_async_copy(update, update_hbm, update_sem)
    last.start()

    @pl.when(late)
    def _():
        for copy in copies:
            copy.wait()

    last.wait()


def per_device(nz, nx, sections, gradient, residual, block_ids, block_counts):
    replicas = nz * nx
    row_count, width = gradient.shape
    cols = width // replicas
    slots = block_ids.shape[1]
    count_total = sections * row_count * width
    f32, bf16, i32 = jnp.float32, jnp.bfloat16, jnp.int32
    dma = pltpu.SemaphoreType.DMA
    blocks = row_count // BLK
    shape = (blocks, BLK, width)
    direct_rows, ext_rows = DIRECT * BLK, (slots - DIRECT) * BLK
    gradient, residual = gradient.reshape(shape), residual.reshape(shape)
    in_hbm = pl.BlockSpec(memory_space=pltpu.HBM)
    in_vmem = pl.BlockSpec(memory_space=pltpu.VMEM)
    in_smem = pl.BlockSpec(memory_space=pltpu.SMEM)
    early_residual = pl.pallas_call(
        functools.partial(ahead, nx),
        out_shape=pltpu.HBM(shape, f32),
        in_specs=[in_hbm, in_hbm, in_hbm, in_smem],
        out_specs=in_hbm,
        scratch_shapes=[pltpu.VMEM(shape, bf16), pltpu.VMEM(shape, f32), pltpu.SMEM((1, slots), i32), dma, dma((2, 4)), dma((4,))],
    )(gradient, residual, block_ids, block_counts)
    new_residual, summed, squares = pl.pallas_call(
        functools.partial(kernel, nz, nx, sections),
        out_shape=(
            pltpu.VMEM(shape, f32), pltpu.VMEM((row_count, cols), f32), pltpu.VMEM((sections * replicas, cols), f32)
        ),
        in_specs=[pl.BlockSpec(memory_space=pltpu.HBM)] * 3 + [pl.BlockSpec(memory_space=pltpu.VMEM)],
        out_specs=(pl.BlockSpec(memory_space=pltpu.VMEM),) * 3,
        scratch_shapes=[
            pltpu.VMEM(shape, bf16),
            pltpu.VMEM(shape, f32),
            pltpu.VMEM((replicas, direct_rows, cols), bf16),
            pltpu.VMEM((nx, nz, ext_rows, cols), bf16),
            pltpu.VMEM((2, LANES), i32),
            pltpu.VMEM((replicas, direct_rows, cols), bf16),
            pltpu.VMEM((nx, nz, ext_rows, cols), bf16),
            pltpu.VMEM((nz, ext_rows, cols), bf16),
            pltpu.VMEM((nz, ext_rows, cols), bf16),
            pltpu.VMEM((nx, LANES), i32),
            pltpu.VMEM((nz, LANES), i32),
            pltpu.VMEM((1, cols), f32),
            pltpu.SMEM((1, slots), i32),
            pltpu.SemaphoreType.REGULAR((nx,)), dma, dma((2, 4)), dma, dma((2,)), dma, dma, dma, dma, dma((2,)), dma((2,)), dma, dma, dma, dma,
        ],
        compiler_params=pltpu.CompilerParams(collective_id=0, has_side_effects=True),
    )(gradient, residual, block_ids, block_counts)
    parts = (pltpu.with_memory_space_constraint(v, pltpu.VMEM) for v in (new_residual, summed, squares))
    new_residual, update = pl.pallas_call(
        functools.partial(finish, count_total, nx),
        out_shape=(pltpu.HBM(shape, f32), pltpu.HBM((row_count, cols), bf16)),
        in_specs=[in_vmem] * 3 + [in_hbm],
        out_specs=(in_hbm, in_hbm),
        scratch_shapes=[pltpu.VMEM((row_count, cols), bf16), dma((4,)), dma],
        input_output_aliases={3: 0},
    )(*parts, early_residual)
    return new_residual.reshape(row_count, width), update


def solution(mesh):
    sections, replicas = mesh.shape["section"], mesh.shape["replica"]
    both = P("section", "replica")
    return jax.shard_map(
        functools.partial(per_device, replicas // NX, NX, sections),
        mesh=mesh,
        in_specs=(both, both, both, both),
        out_specs=(both, both),
        check_vma=False,
    )
```
